32 devices in a mesh: parts: 2 (over y), seq: 4 (over z), head: 4 (over x, core).
Axes of the slice: x: 2, y: 2, z: 4, core: 2. Of those that a mesh axis runs over, the one named last changes fastest.
Arguments:
- queries: bfloat16 [256, 8192], P(('parts', 'seq'), 'head'), parts along dimension 0, may hold values from -110 to 110
- root_keys: bfloat16 [16384, 1024], P(('parts', 'seq'), 'head'), parts along dimension 0, may hold values from -6 to 6
- root_values: bfloat16 [16384, 1024], P(('parts', 'seq'), 'head'), parts along dimension 0, may hold values from -6 to 6
- branch_keys: bfloat16 [16, 2048, 1024], P(('parts', 'seq'), None, 'head'), parts along dimension 0, may hold values from -6 to 6
- branch_values: bfloat16 [16, 2048, 1024], P(('parts', 'seq'), None, 'head'), parts along dimension 0, may hold values from -6 to 6
- branch_id: int32 [256, 1], P('parts'), parts along dimension 0, may hold values from 0 to 7; in each aligned block of 128 rows (0 to 127, 128 to 255, ...) at most 32 rows name the same one
- doc_len: int32 [16], P('parts'), parts along dimension 0, may hold values from 1 to 2048, 10240 in all
Outputs:
- attended: bfloat16 [256, 8192], P(('parts', 'seq'), 'head'), parts along dimension 0
The draws below stay inside these ranges and needn't reach their ends.
There are 2 independent parts, one for each index of `parts`. The reference program is written for one: setup_inputs(seed, part) draws one part's arguments, and reference() takes and returns one part's arrays. A program takes and returns all parts, laid end to end along the dimension named above; each array names one. Nothing has to cross between parts.
Inputs may be any that keep to these rules, and one draw needn't show every extreme that they name: `branch_id`: each of the 8 branches is named by at most 32 rows, a bound that some block reaches. `doc_len`: the 8 lengths of ONE part sum to 10240 and the largest of them is exactly 2048; the printed array holds all parts end to end, so its whole sum is that total times the number of parts.
All inputs are finite; a program needn't handle non-finite values.
Results may differ from the reference program's by a relative error of at most 0.008.
Values may be sent and summed in bfloat16 or wider, within the bound.
No kernel may reach another device: no remote copies, remote signals or barrier semaphores. Data moves between devices by JAX's collectives and lax.ppermute only.
A program may use at most 64 MiB of HBM per device.

```python
import math
import jax
import jax.numpy as jnp
import numpy as np
from jax import lax

QHEADS = 64
KVHEADS = 8
HEAD_DIM = 128
BRANCH_LEN = 2048
ROOT = 8192
ROWS = 128
BRANCHES = 8
MOST_ROWS = 32


def draw_queries(key, part):
    extent = (ROWS, QHEADS * HEAD_DIM)
    result = jnp.clip(jax.random.normal(key, extent, jnp.float32), -6.0, 6.0)
    return result.astype(jnp.bfloat16)


def shard_levels(stream_key, dims, cuts, low, high):
    loudness = 1.0
    for axis_at, blocks in cuts:
        steps = jax.random.uniform(jax.random.fold_in(jax.random.fold_in(stream_key, 6), axis_at), (blocks,), jnp.float32, low / len(cuts), high / len(cuts))
        loudness = loudness * jnp.repeat(jnp.exp(steps), dims[axis_at] // blocks).reshape((-1,) + (1,) * (len(dims) - 1 - axis_at))
    return loudness


def profile(amount, total, limit, skew):
    weights = [(1 << 20) // math.isqrt(standing ** skew) + 1 for standing in range(2, amount + 1)]
    surplus, given = total - limit - (amount - 1), [1] * (amount - 1)
    while surplus > 0:
        movable = [i for i in range(amount - 1) if given[i] < limit]
        mass, left = sum([weights[i] for i in movable]), surplus
        for i in movable:
            extra = min(limit - given[i], max(1, left * weights[i] // mass), surplus)
            given[i] = given[i] + extra
            surplus = surplus - extra
    return np.array([limit] + given)


def ragged(rng, amount, total, reach, skew):
    if amount == 2:
        one = jax.random.randint(rng, (), max(1, total - reach), min(reach, total - 1) + 1)
        return jnp.stack([one, total - one])
    tallies = jnp.asarray(profile(amount, total, reach, skew), jnp.int32)
    twos = (amount - 1) // 2
    giver, sink = tallies[1:1 + 2 * twos:2], tallies[2:2 + 2 * twos:2]
    slack = jnp.minimum(giver - 1, reach - sink)
    shifted = jax.random.randint(jax.random.fold_in(rng, 1), (twos,), 0, 1 << 20) % (slack + 1)
    tallies = tallies.at[1:1 + 2 * twos:2].set(giver - shifted).at[2:2 + 2 * twos:2].set(sink + shifted)
    return tallies[jax.random.permutation(jax.random.fold_in(rng, 2), amount)]


def assign_block(stream_key, own, number, rows, number_of, top, most, slope):
    sequence = jax.random.permutation(stream_key, number_of)
    heavy_load, ordinary = portions_of(number_of, rows * top, most, slope, True), portions_of(number_of, rows * top, most, slope, False)
    places = jnp.arange(number_of)

    def named(sizes, rotation):
        used = int((sizes > 0).sum())
        fixed = max(1, used // 4)
        shifted = fixed + (places - fixed + rotation * (used - fixed)) % max(1, number_of - fixed)
        return jnp.zeros((number_of,), jnp.int32).at[sequence[jnp.where(places < fixed, places, shifted)]].set(jnp.asarray(sizes, jnp.int32))

    sizes = jnp.where(number % 4 == 0, named(heavy_load, number // 4), named(ordinary, number - number // 4 - 1))
    mixed = jax.random.permutation(jax.random.fold_in(own, 3), number_of)
    giver, receiver = mixed[0:number_of // 2 * 2:2], mixed[1:number_of // 2 * 2:2]
    room = jnp.minimum(sizes[giver] - 1, most - sizes[receiver]) // 2
    room = jnp.where((giver == sequence[0]) | (receiver == sequence[0]) | (sizes[receiver] == 0), 0, jnp.maximum(room, 0))
    shifted = jax.random.randint(jax.random.fold_in(own, 4), (number_of // 2,), 0, 1 << 20) % (room + 1)
    sizes = sizes.at[giver].add(-shifted).at[receiver].add(shifted)
    members = jnp.searchsorted(jnp.cumsum(sizes), jnp.arange(rows * top), side="right").astype(jnp.int32)
    grid = members.reshape(top, rows).T
    grid = grid[jax.random.permutation(jax.random.fold_in(own, 1), rows)]
    rotation = jax.random.randint(jax.random.fold_in(own, 2), (rows, 1), 0, top)
    return jnp.take_along_axis(grid, (jnp.arange(top)[None, :] + rotation) % top, axis=1)


def portions_of(amount, total, reach, lean, full):
    portions = [(1 << 20) // math.isqrt(grade ** lean) + 1 for grade in range(1, amount + 1)]
    largest = reach if full else min(reach, max(-(-total // amount), total * portions[0] // sum(portions)))
    least = 1 if total - largest >= amount - 1 else 0
    given, surplus = [largest] + [least] * (amount - 1), total - largest - least * (amount - 1)
    while surplus > 0:
        movable = [i for i in range(1, amount) if given[i] < largest] or [i for i in range(1, amount) if given[i] < reach]
        mass, budget = sum([portions[i] for i in movable]), surplus
        for i in movable:
            extra = min(reach - given[i], max(1, budget * portions[i] // mass), surplus)
            given[i] = given[i] + extra
            surplus = surplus - extra
    return np.array(given)


def centred(rng, dims, scale, reach, cuts=(), kind=jnp.bfloat16):
    level = shard_levels(rng, dims, cuts, -0.22, 0.18) if cuts else 1.0
    values = jax.random.normal(rng, dims, jnp.float32) * scale * level
    return jnp.minimum(jnp.maximum(values, -reach), reach).astype(kind)


def setup_inputs(seed: int = 0, part: int = 0) -> dict:
    keys = jax.random.split(jax.random.key(seed), 8)
    part_keys = jax.random.split(jax.random.fold_in(keys[7], part), 8)
    queries = draw_queries(jax.random.fold_in(jax.random.fold_in(keys[7], part), 71), part)
    root_keys = centred(part_keys[1], (ROOT, KVHEADS * HEAD_DIM), 1.0, 6.0, ((0, 4), (1, 4)))
    root_values = centred(part_keys[2], (ROOT, KVHEADS * HEAD_DIM), 1.0, 6.0, ((0, 4), (1, 4)))
    branch_keys = centred(part_keys[3], (BRANCHES, BRANCH_LEN, KVHEADS * HEAD_DIM), 1.0, 6.0, ((0, 4), (2, 4)))
    branch_values = centred(part_keys[4], (BRANCHES, BRANCH_LEN, KVHEADS * HEAD_DIM), 1.0, 6.0, ((0, 4), (2, 4)))
    branch_id_keys = jax.random.split(jax.random.fold_in(part_keys[5], 1), ROWS // ROWS)
    branch_id_turns = jax.random.permutation(jax.random.fold_in(part_keys[5], 3), ROWS // ROWS)
    branch_id = jax.vmap(lambda own, number: assign_block(jax.random.fold_in(part_keys[5], 2), own, number, ROWS, BRANCHES, 1, MOST_ROWS, 2))(branch_id_keys, branch_id_turns).reshape((ROWS, 1))
    doc_len = ragged(part_keys[6], BRANCHES, BRANCHES * BRANCH_LEN * 5 // 8, BRANCH_LEN, 2).astype(jnp.int32)
    return {"queries": queries, "root_keys": root_keys, "root_values": root_values, "branch_keys": branch_keys, "branch_values": branch_values, "branch_id": branch_id, "doc_len": doc_len}


masked_score = -1.0e30


def attend(query_head_rows, key_tile_rows, value_tile_rows, usable):
    logit_scale = HEAD_DIM ** -0.5
    logit_scores = jnp.einsum('mfsa,nfa->mfsn', query_head_rows.astype(jnp.float32), key_tile_rows.astype(jnp.float32)) * logit_scale
    keep = usable[:, None, None, :]
    logit_scores = jnp.where(keep, logit_scores, masked_score)
    row_max = jnp.max(logit_scores, axis=-1)
    softmax_weights = jnp.where(keep, jnp.exp(logit_scores - row_max[..., None]), 0.0)
    row_sum = jnp.sum(softmax_weights, axis=-1)
    weighted_values = jnp.einsum('taoz,zah->taoh', softmax_weights.astype(jnp.bfloat16).astype(jnp.float32), value_tile_rows.astype(jnp.float32))
    return row_max, row_sum, weighted_values


def combine(first, second):
    row_max = jnp.maximum(first[0], second[0])
    factor_a = jnp.exp(first[0] - row_max)
    factor_b = jnp.exp(second[0] - row_max)
    return (row_max, first[1] * factor_a + second[1] * factor_b,
            first[2] * factor_a[..., None] + second[2] * factor_b[..., None])


def reference(queries, root_keys, root_values, branch_keys, branch_values, branch_id, doc_len):
    group = QHEADS // KVHEADS
    query_head_rows = queries.reshape(ROWS, KVHEADS, group, HEAD_DIM)
    block_len = min(1024, ROOT)
    key_blocks = root_keys.reshape(ROOT // block_len, block_len, KVHEADS, HEAD_DIM)
    value_blocks = root_values.reshape(ROOT // block_len, block_len, KVHEADS, HEAD_DIM)
    starts = (jnp.full((ROWS, KVHEADS, group), masked_score, jnp.float32),
              jnp.zeros((ROWS, KVHEADS, group), jnp.float32),
              jnp.zeros((ROWS, KVHEADS, group, HEAD_DIM), jnp.float32))

    def root_step(carry, pair):
        usable = jnp.ones((1, block_len), bool)
        return combine(carry, attend(query_head_rows, pair[0], pair[1], usable)), None

    root_part, _ = lax.scan(root_step, starts, (key_blocks, value_blocks))

    def one_branch(branch):
        chosen = jnp.argsort((branch_id[:, 0] != branch).astype(jnp.int32), stable=True)[:MOST_ROWS].astype(jnp.int32)
        row_live = branch_id[chosen, 0] == branch
        key_live = jnp.arange(BRANCH_LEN) < doc_len[branch]
        usable = row_live[:, None] & key_live[None, :]
        key_tile_rows = lax.dynamic_index_in_dim(branch_keys, branch, 0, keepdims=False).reshape(BRANCH_LEN, KVHEADS, HEAD_DIM)
        value_tile_rows = lax.dynamic_index_in_dim(branch_values, branch, 0, keepdims=False).reshape(BRANCH_LEN, KVHEADS, HEAD_DIM)
        result = attend(query_head_rows[chosen], key_tile_rows, value_tile_rows, usable)
        target = jnp.where(row_live, chosen, ROWS).astype(jnp.int32)
        return result + (target,)

    mapped = lax.map(one_branch, jnp.arange(BRANCHES, dtype=jnp.int32))
    targets = mapped[3].reshape(-1)
    branch_part = (
        starts[0].at[targets].set(mapped[0].reshape(-1, KVHEADS, group), mode="drop"),
        starts[1].at[targets].set(mapped[1].reshape(-1, KVHEADS, group), mode="drop"),
        starts[2].at[targets].set(mapped[2].reshape(-1, KVHEADS, group, HEAD_DIM), mode="drop"))
    joined = combine(root_part, branch_part)
    attended = joined[2] / joined[1][..., None]
    return attended.astype(jnp.bfloat16).reshape(ROWS, QHEADS * HEAD_DIM)
```

```python
import functools
import math

import jax
import jax.numpy as jnp
from jax import lax
from jax.experimental import pallas as pl
from jax.experimental.pallas import tpu as pltpu
from jax.sharding import PartitionSpec as P

QHEADS = 64
KVHEADS = 8
HEAD_DIM = 128
GROUP = QHEADS // KVHEADS
LOW = -1.0e30
SCALE = HEAD_DIM ** -0.5 * math.log2(math.e)
STAT = 16


def dot(a, b, dims=(((1,), (0,)), ((), ()))):
    return lax.dot_general(a, b, dims, preferred_element_type=jnp.float32)


def pieces(x):
    hi = x.astype(jnp.bfloat16)
    rest = x - hi.astype(jnp.float32)
    mid = rest.astype(jnp.bfloat16)
    low = (rest - mid.astype(jnp.float32)).astype(jnp.bfloat16)
    return hi, mid, low


def attend(query, keys, values, score_ref, weight_ref, bias=None):
    rows = query.shape[0]
    total = score_ref.shape[1]
    tile = 256
    best = None
    for j in range(total // tile):
        s = dot(query, keys(j, tile), (((1,), (1,)), ((), ())))
        if bias is not None:
            s = s + bias(j, tile)
        score_ref[:, j * tile:(j + 1) * tile] = s
        for part in range(tile // HEAD_DIM):
            t = s[:, part * HEAD_DIM:(part + 1) * HEAD_DIM]
            best = t if best is None else jnp.maximum(best, t)
    peak = jnp.broadcast_to(jnp.max(best, axis=1, keepdims=True) * SCALE, (rows, HEAD_DIM))
    peak2 = jnp.concatenate([peak, peak], axis=1)
    for j in range(total // tile):
        w = jnp.exp2(score_ref[:, j * tile:(j + 1) * tile] * SCALE - peak2)
        weight_ref[:, j * tile:(j + 1) * tile] = w.astype(jnp.bfloat16)
    tiles = [jnp.concatenate([values(j, tile), jnp.ones((tile, HEAD_DIM), jnp.bfloat16)], axis=1) for j in range(total // tile)]
    out = dot(weight_ref[...], jnp.concatenate(tiles, axis=0))
    denominator = out[:, HEAD_DIM:]
    return out[:, :HEAD_DIM] / denominator, peak + jnp.log2(denominator)


def stack_heads(chunk, f):
    at = f * GROUP
    return jnp.concatenate([chunk[:, (at + h) * HEAD_DIM:(at + h + 1) * HEAD_DIM] for h in range(GROUP)], axis=0)


def write_share(out_ref, first, f, output, level, row_dev, heads):
    out_ref[first + f * GROUP * row_dev:first + (f + 1) * GROUP * row_dev, :] = output.astype(jnp.bfloat16)
    lane = lax.broadcasted_iota(jnp.int32, (row_dev, HEAD_DIM), 1)
    stat = jnp.zeros((row_dev, HEAD_DIM), jnp.float32)
    for h in range(GROUP):
        stat = jnp.where(lane % heads == f * GROUP + h, level[h * row_dev:(h + 1) * row_dev, :], stat)
    return stat


def write_stats(out_ref, first, stat, row_dev, heads):
    lane = lax.broadcasted_iota(jnp.int32, (row_dev, HEAD_DIM), 1)
    hi, mid, low = pieces(stat)
    zero = jnp.zeros_like(stat)
    packed = jnp.where(lane < heads, hi.astype(jnp.float32), jnp.where(lane < 2 * heads, mid.astype(jnp.float32), jnp.where(lane < 3 * heads, low.astype(jnp.float32), zero)))
    half = row_dev // 2
    both = packed[:half] + pltpu.roll(packed[half:], HEAD_DIM // 2, 1)
    out_ref[first + heads * row_dev:first + heads * row_dev + half, :] = both.astype(jnp.bfloat16)


def work(me_ref, doc_ref, id_ref, rk_ref, rv_ref, bk_ref, bv_ref, *rest, shares, kv_local, most_rows):
    q_refs = rest[:shares]
    out_refs = rest[shares:2 * shares]
    score_ref, weight_ref, pick_ref, level_ref, branch_ref = rest[2 * shares:]
    row_dev = q_refs[0].shape[0]
    rows = id_ref.shape[0]
    branch_dev = bk_ref.shape[0]
    heads = kv_local * GROUP
    me = me_ref[0]

    ids = id_ref[...]
    before = (lax.broadcasted_iota(jnp.int32, (rows, rows), 0) > lax.broadcasted_iota(jnp.int32, (rows, rows), 1)).astype(jnp.bfloat16)
    for b in range(branch_dev):
        named = ids == me * branch_dev + b
        named_wide = jnp.broadcast_to(named.astype(jnp.float32), (rows, HEAD_DIM))
        rank = dot(before, named_wide.astype(jnp.bfloat16))[:, :most_rows]
        slot = lax.broadcasted_iota(jnp.int32, (rows, most_rows), 1).astype(jnp.float32)
        chosen = jnp.where((rank == slot) & (named_wide[:, :most_rows] > 0.0), 1.0, 0.0)
        pick_ref[b] = chosen.astype(jnp.bfloat16)

    for f in range(kv_local):
        cut = slice(f * HEAD_DIM, (f + 1) * HEAD_DIM)
        wide = slice(f * GROUP * HEAD_DIM, (f + 1) * GROUP * HEAD_DIM)
        for b in range(branch_dev):
            picked = None
            for k in range(shares):
                source = lax.rem(me - k + shares, shares)
                sel = pick_ref[b, pl.ds(pl.multiple_of(source * row_dev, row_dev), row_dev), :]
                part = dot(sel, q_refs[k][:, wide], (((0,), (0,)), ((), ())))
                picked = part if picked is None else picked + part
            query = stack_heads(picked.astype(jnp.bfloat16), 0)
            length = doc_ref[me * branch_dev + b]

            def bias(j, tile):
                slot = lax.broadcasted_iota(jnp.int32, (1, tile), 1) + j * tile
                return jnp.where(slot < length, 0.0, LOW)

            output, level = attend(query, lambda j, t: bk_ref[b, j * t:(j + 1) * t, cut], lambda j, t: bv_ref[b, j * t:(j + 1) * t, cut], score_ref, weight_ref, bias)
            for h in range(GROUP):
                at = slice(h * most_rows, (h + 1) * most_rows)
                to = slice((f * GROUP + h) * HEAD_DIM, (f * GROUP + h + 1) * HEAD_DIM)
                branch_ref[b * most_rows:(b + 1) * most_rows, to] = output[at]
                level_ref[b * most_rows:(b + 1) * most_rows, to] = level[at]

    for k in range(shares):
        source = lax.rem(me - k + shares, shares)
        at = pl.ds(pl.multiple_of(source * row_dev, row_dev), row_dev)
        pick = jnp.concatenate([pick_ref[b, at, :] for b in range(branch_dev)], axis=1)
        has = jnp.sum(pick.astype(jnp.float32), axis=1, keepdims=True) > 0.0
        stat = None
        for f in range(kv_local):
            cut = slice(f * HEAD_DIM, (f + 1) * HEAD_DIM)
            wide = slice(f * GROUP * HEAD_DIM, (f + 1) * GROUP * HEAD_DIM)
            query = stack_heads(q_refs[k], f)
            output, level = attend(query, lambda j, t: rk_ref[j * t:(j + 1) * t, cut], lambda j, t: rv_ref[j * t:(j + 1) * t, cut], score_ref, weight_ref)
            b_out = sum(dot(pick, p) for p in pieces(branch_ref[:, wide])[:2])
            b_level = sum(dot(pick, p) for p in pieces(level_ref[:, wide]))
            b_level = jnp.where(has, b_level, LOW)
            b_out, b_level = stack_heads(b_out, 0), stack_heads(b_level, 0)
            top = jnp.maximum(level, b_level)
            ours, theirs = jnp.exp2(level - top), jnp.exp2(b_level - top)
            both = ours + theirs
            merged = (output * ours + b_out * theirs) / both
            here = write_share(out_refs[k], 0, f, merged, top + jnp.log2(both), row_dev, heads)
            stat = here if stat is None else stat + here
        write_stats(out_refs[k], 0, stat, row_dev, heads)


def join(*refs, heads):
    share_refs, out_ref = refs[:-1], refs[-1]
    row_dev = out_ref.shape[0]
    half = row_dev // 2
    levels = []
    for ref in share_refs:
        s = ref[heads * row_dev:heads * row_dev + half, :].astype(jnp.float32)
        levels.append(s + pltpu.roll(s, HEAD_DIM - heads, 1) + pltpu.roll(s, HEAD_DIM - 2 * heads, 1))
    top = functools.reduce(jnp.maximum, levels)
    parts = [jnp.exp2(x - top) for x in levels]
    whole = functools.reduce(jnp.add, parts)
    parts = [x / whole for x in parts]
    for h in range(heads):
        result = None
        for ref, part in zip(share_refs, parts):
            factor = jnp.concatenate([jnp.broadcast_to(part[:, at:at + 1], (half, HEAD_DIM)) for at in (h, HEAD_DIM // 2 + h)], axis=0)
            term = ref[h * row_dev:(h + 1) * row_dev, :].astype(jnp.float32) * factor
            result = term if result is None else result + term
        out_ref[:, h * HEAD_DIM:(h + 1) * HEAD_DIM] = result.astype(jnp.bfloat16)


VMEM = pl.BlockSpec(memory_space=pltpu.VMEM)
SMEM = pl.BlockSpec(memory_space=pltpu.SMEM)


def body(queries, root_keys, root_values, branch_keys, branch_values, branch_id, doc_len):
    shares = lax.axis_size("seq")
    me = lax.axis_index("seq").astype(jnp.int32)
    row_dev, width = queries.shape
    heads = width // HEAD_DIM
    kv_local = root_keys.shape[1] // HEAD_DIM
    branch_dev, branch_len, _ = branch_keys.shape
    most_rows = 2 * row_dev // branch_dev

    def shift(x, k):
        return lax.ppermute(x, "seq", [(i, (i + k) % shares) for i in range(shares)])

    gathered = [queries] + [shift(queries, k) for k in range(1, shares)]
    share_shape = jax.ShapeDtypeStruct((heads * row_dev + row_dev // 2, HEAD_DIM), jnp.bfloat16)
    block = GROUP * row_dev
    sent = pl.pallas_call(
        functools.partial(work, shares=shares, kv_local=kv_local, most_rows=most_rows),
        out_shape=[share_shape] * shares,
        in_specs=[SMEM, SMEM] + [VMEM] * (5 + shares),
        out_specs=[VMEM] * shares,
        scratch_shapes=[
            pltpu.VMEM((block, root_keys.shape[0]), jnp.float32),
            pltpu.VMEM((block, root_keys.shape[0]), jnp.bfloat16),
            pltpu.VMEM((branch_dev, branch_id.shape[0], most_rows), jnp.bfloat16),
            pltpu.VMEM((branch_dev * most_rows, width), jnp.float32),
            pltpu.VMEM((branch_dev * most_rows, width), jnp.float32),
        ],
        name="work",
    )(me[None], doc_len, branch_id, root_keys, root_values, branch_keys, branch_values, *gathered)
    received = [sent[0]] + [shift(sent[k], shares - k) for k in range(1, shares)]
    return pl.pallas_call(
        functools.partial(join, heads=heads),
        out_shape=jax.ShapeDtypeStruct((row_dev, width), jnp.bfloat16),
        in_specs=[VMEM] * shares,
        out_specs=VMEM,
        name="join",
    )(*received)


def solution(mesh):
    rows = P(("parts", "seq"), "head")
    in_specs = (
        rows,
        rows,
        rows,
        P(("parts", "seq"), None, "head"),
        P(("parts", "seq"), None, "head"),
        P("parts", None),
        P("parts"),
    )
    return jax.shard_map(body, mesh=mesh, in_specs=in_specs, out_specs=rows, check_vma=False)
```

```python
import functools
import math

import jax
import jax.numpy as jnp
from jax import lax
from jax.experimental import pallas as pl
from jax.experimental.pallas import tpu as pltpu
from jax.sharding import PartitionSpec as P

QHEADS = 64
KVHEADS = 8
HEAD_DIM = 128
GROUP = QHEADS // KVHEADS
LOW = -1.0e30
SCALE = HEAD_DIM ** -0.5 * math.log2(math.e)
TILE = 256
VMEM_BYTES = 20 * 2 ** 20


def dot(a, b, dims=(((1,), (0,)), ((), ()))):
    return lax.dot_general(a, b, dims, preferred_element_type=jnp.float32)


def pieces(x):
    hi = x.astype(jnp.bfloat16)
    rest = x - hi.astype(jnp.float32)
    mid = rest.astype(jnp.bfloat16)
    low = (rest - mid.astype(jnp.float32)).astype(jnp.bfloat16)
    return hi, mid, low


def pipeline(blocks, score_ref):
    query, best = {}, {}

    def tiles(i):
        return [slice(at, at + TILE) for at in range(0, blocks[i][4], TILE)] if i < len(blocks) else []

    def score(i, at):
        if i not in query:
            query[i] = blocks[i][0]()
        s = dot(query[i], blocks[i][1](at), (((1,), (1,)), ((), ())))
        if blocks[i][3] is not None:
            s = s + blocks[i][3](at)
        score_ref[i % 2, :, at] = s
        for part in range(TILE // HEAD_DIM):
            t = s[:, part * HEAD_DIM:(part + 1) * HEAD_DIM]
            best[i] = jnp.maximum(best[i], t) if i in best else t

    for at in tiles(0):
        score(0, at)
    for i, (_, _, values, _, _, finish) in enumerate(blocks):
        peak = jnp.broadcast_to(jnp.max(best[i], axis=1, keepdims=True) * SCALE, best[i].shape)
        wide = jnp.concatenate([peak] * (TILE // HEAD_DIM), axis=1)
        ahead = tiles(i + 1)
        out = None
        for at in tiles(i):
            for later in ahead[:1]:
                score(i + 1, later)
            ahead = ahead[1:]
            w = jnp.exp2(score_ref[i % 2, :, at] * SCALE - wide).astype(jnp.bfloat16)
            part = dot(w, jnp.concatenate([values(at), jnp.ones((TILE, HEAD_DIM), jnp.bfloat16)], axis=1))
            out = part if out is None else out + part
        for later in ahead:
            score(i + 1, later)
        whole = out[:, HEAD_DIM:]
        finish(out[:, :HEAD_DIM] / whole, peak + jnp.log2(whole))


def stack_heads(chunk, first=0):
    return jnp.concatenate([chunk[:, (first + h) * HEAD_DIM:(first + h + 1) * HEAD_DIM] for h in range(GROUP)], axis=0)


def compact(levels):
    rows = next(iter(levels.values())).shape[0] // GROUP
    lane = lax.broadcasted_iota(jnp.int32, (rows, HEAD_DIM), 1)
    result = jnp.zeros((rows, HEAD_DIM), jnp.float32)
    for f, level in levels.items():
        for h in range(GROUP):
            result = jnp.where(lane == f * GROUP + h, level[h * rows:(h + 1) * rows, :], result)
    return result


def spread(stat, h, rows):
    return jnp.broadcast_to(stat[:, h:h + 1], (rows, HEAD_DIM))


def roots(query, rk_ref, rv_ref, heads, finish):
    outputs, levels = {}, {}

    def block(f):
        cut = slice(f * HEAD_DIM, (f + 1) * HEAD_DIM)

        def done(output, level):
            outputs[f], levels[f] = output, level
            if len(levels) == len(heads):
                finish(outputs, compact(levels))

        return (lambda: query(f), lambda at: rk_ref[at, cut], lambda at: rv_ref[at, cut], None, rk_ref.shape[0], done)

    return [block(f) for f in heads]


def store(out_ref, level_ref):
    def finish(outputs, level):
        for f, output in outputs.items():
            out_ref[f] = output
        level_ref[...] = level

    return finish


def own(*rest, kv_local):
    sources, rest = rest[:7], rest[7:]
    rk_ref, rv_ref, bk_ref, bv_ref, pick_ref, bias_ref, out_ref, level_ref, score_ref, id_ref, q_ref, doc_ref, arrived = rest
    loads = [pltpu.make_async_copy(source, target, arrived.at[n]) for n, (source, target) in enumerate(zip(sources, (id_ref, q_ref, rk_ref, doc_ref, rv_ref, bk_ref, bv_ref)))]
    for load in loads[:5]:
        load.start()
    branch_dev, rows, most_rows = pick_ref.shape
    me = lax.axis_index("seq").astype(jnp.int32)
    loads[3].wait()
    slot = lax.broadcasted_iota(jnp.int32, (1, bias_ref.shape[1]), 1)
    for b in range(branch_dev):
        bias_ref[b:b + 1, :] = jnp.where(slot < doc_ref[me * branch_dev + b], 0.0, LOW)
    loads[0].wait()
    ids = id_ref[...]
    before = jnp.where(lax.broadcasted_iota(jnp.int32, (rows, rows), 0) < lax.broadcasted_iota(jnp.int32, (rows, rows), 1), 1.0, 0.0).astype(jnp.bfloat16)
    slot = lax.broadcasted_iota(jnp.int32, (most_rows, rows), 0).astype(jnp.float32)
    unit = jnp.where(lax.broadcasted_iota(jnp.int32, (most_rows, most_rows), 0) == lax.broadcasted_iota(jnp.int32, (most_rows, most_rows), 1), 1.0, 0.0).astype(jnp.bfloat16)
    for b in range(branch_dev):
        named = jnp.broadcast_to(jnp.where(ids == me * branch_dev + b, 1.0, 0.0), (most_rows, rows))
        rank = dot(named.astype(jnp.bfloat16), before)
        chosen = jnp.where((rank == slot) & (named > 0.0), 1.0, 0.0).astype(jnp.bfloat16)
        pick_ref[b] = dot(chosen, unit, (((0,), (0,)), ((), ()))).astype(jnp.bfloat16)
    for load in loads[1:3] + loads[4:5]:
        load.wait()
    for load in loads[5:]:
        load.start()
    pipeline(roots(lambda f: stack_heads(q_ref, f * GROUP), rk_ref, rv_ref, range(kv_local), store(out_ref, level_ref)), score_ref)
    for load in loads[5:]:
        load.wait()


def root(q_ref, rk_ref, rv_ref, out_ref, level_ref, score_ref, *, kv_local):
    pipeline(roots(lambda f: stack_heads(q_ref, f * GROUP), rk_ref, rv_ref, range(kv_local), store(out_ref, level_ref)), score_ref)


def picks(pick_ref, key, row_dev):
    source = lax.axis_index("seq").astype(jnp.int32) ^ key
    at = pl.ds(pl.multiple_of(source * row_dev, row_dev), row_dev)
    return [pick_ref[b, at, :] for b in range(pick_ref.shape[0])]


def merge(share_ref, pick, outputs, level, branch_refs, b_level):
    row_dev = level.shape[0]
    pick = jnp.concatenate(pick, axis=1)
    has = jnp.sum(pick.astype(jnp.float32), axis=1, keepdims=True) > 0.0
    found = dot(pick, b_level)
    b_level = jnp.where(has, found[:, :HEAD_DIM] + found[:, HEAD_DIM:2 * HEAD_DIM] + found[:, 2 * HEAD_DIM:], LOW)
    top = jnp.maximum(level, b_level)
    ours, theirs = jnp.exp2(level - top), jnp.exp2(b_level - top)
    both = ours + theirs
    ours, theirs = ours / both, theirs / both
    for n, (f, output) in enumerate(outputs.items()):
        b_out = dot(pick, branch_refs[f][...])
        for g in range(GROUP):
            h = f * GROUP + g
            at = (n * GROUP + g) * row_dev
            ahead = output[g * row_dev:(g + 1) * row_dev, :] * spread(ours, h, row_dev)
            share_ref[at:at + row_dev, :] = (ahead + b_out[:, g * HEAD_DIM:(g + 1) * HEAD_DIM] * spread(theirs, h, row_dev)).astype(jnp.bfloat16)
    lane = lax.broadcasted_iota(jnp.int32, (row_dev, HEAD_DIM), 1)
    here = functools.reduce(jnp.logical_or, [(lane >= f * GROUP) & (lane < (f + 1) * GROUP) for f in outputs])
    stat = jnp.where(here, top + jnp.log2(both), 0.0)
    heads = len(branch_refs) * GROUP
    stat = stat + pltpu.roll(stat, heads, 1) + pltpu.roll(stat, 2 * heads, 1)
    hi, mid, low = [piece.astype(jnp.float32) for piece in pieces(stat)]
    packed = jnp.where(lane < heads, hi, jnp.where(lane < 2 * heads, mid, low))
    half = row_dev // 2
    share_ref[len(outputs) * GROUP * row_dev:, :] = (packed[:half] + pltpu.roll(packed[half:], HEAD_DIM // 2, 1)).astype(jnp.bfloat16)


def branch_blocks(pick_ref, bias_ref, bk_ref, bv_ref, q_refs, rows_ref, branch_ref, keys, f, finish):
    row_dev = q_refs[0].shape[0]
    branch_dev, _, most_rows = pick_ref.shape
    part = rows_ref.shape[1]
    cut = slice(f * HEAD_DIM, (f + 1) * HEAD_DIM)
    me = lax.axis_index("seq").astype(jnp.int32)
    for k, q_ref in zip(keys, q_refs):
        at = pl.ds(pl.multiple_of((me ^ k) * row_dev, row_dev), row_dev)
        rows_ref[at, :] = q_ref[...] if k == keys[-1] else q_ref[:, f * part:(f + 1) * part]
    named = jnp.concatenate([pick_ref[b] for b in range(branch_dev)], axis=1)
    picked = dot(named, rows_ref[...], (((0,), (0,)), ((), ()))).astype(jnp.bfloat16)
    levels = []

    def block(b):
        def done(output, level):
            for h in range(GROUP):
                branch_ref[b * most_rows:(b + 1) * most_rows, h * HEAD_DIM:(h + 1) * HEAD_DIM] = output[h * most_rows:(h + 1) * most_rows].astype(jnp.bfloat16)
            levels.append(compact({f: level}))
            if len(levels) == branch_dev:
                finish(jnp.concatenate(levels, axis=0))

        return (lambda: stack_heads(picked[b * most_rows:(b + 1) * most_rows]), lambda at: bk_ref[b, at, cut], lambda at: bv_ref[b, at, cut], lambda at: bias_ref[b:b + 1, at], bk_ref.shape[1], done)

    return [block(b) for b in range(branch_dev)]


def branch(pick_ref, bias_ref, bk_ref, bv_ref, out_ref, level_ref, *rest, keys, f, key, kv_local):
    branch_refs, rest = rest[:f], rest[f:]
    total_refs, rest = rest[:min(f, 1)], rest[min(f, 1):]
    q_refs = rest[:len(keys)]
    share_ref, branch_ref, total_ref, score_ref, rows_ref = rest[len(keys):]

    def finish(level):
        total = jnp.concatenate(pieces(level), axis=1)
        for ref in total_refs:
            total = total + ref[...]
        total_ref[...] = total

    pipeline(branch_blocks(pick_ref, bias_ref, bk_ref, bv_ref, q_refs, rows_ref, branch_ref, keys, f, finish), score_ref)
    every = [*branch_refs, branch_ref] + [None] * (kv_local - 1 - f)
    merge(share_ref, picks(pick_ref, key, level_ref.shape[0]), {f: out_ref[f]}, level_ref[...], every, total_ref[...])


def share(pick_ref, b_level_ref, rk_ref, rv_ref, *rest, key, kv_local):
    branch_refs, q_refs, share_ref, score_ref = rest[:kv_local], rest[kv_local:2 * kv_local], rest[-2], rest[-1]

    def finish(outputs, level):
        merge(share_ref, picks(pick_ref, key, level.shape[0]), outputs, level, branch_refs, b_level_ref[...])

    pipeline(roots(lambda f: stack_heads(q_refs[f]), rk_ref, rv_ref, range(kv_local), finish), score_ref)


def given(pick_ref, b_level_ref, out_ref, level_ref, *rest, key):
    branch_refs, share_ref = rest[:-1], rest[-1]
    merge(share_ref, picks(pick_ref, key, level_ref.shape[0]), {f: out_ref[f] for f in range(len(branch_refs))}, level_ref[...], branch_refs, b_level_ref[...])


def join(*refs, heads, counts):
    out_ref = refs[-1]
    row_dev = out_ref.shape[0]
    half = row_dev // 2
    groups, at = [], 0
    for count in counts:
        groups.append(refs[at:at + count])
        at += count
    levels = []
    for group in groups:
        s = sum(ref[heads // len(group) * row_dev:, :].astype(jnp.float32) for ref in group)
        levels.append(s + pltpu.roll(s, HEAD_DIM - heads, 1) + pltpu.roll(s, HEAD_DIM - 2 * heads, 1))
    top = functools.reduce(jnp.maximum, levels)
    parts = [jnp.exp2(x - top) for x in levels]
    whole = functools.reduce(jnp.add, parts)
    parts = [x / whole for x in parts]
    for h in range(heads):
        result = None
        for group, part in zip(groups, parts):
            each = heads // len(group)
            factor = jnp.concatenate([spread(part, h, half), spread(part, HEAD_DIM // 2 + h, half)], axis=0)
            term = group[h // each][h % each * row_dev:(h % each + 1) * row_dev, :].astype(jnp.float32) * factor
            result = term if result is None else result + term
        out_ref[:, h * HEAD_DIM:(h + 1) * HEAD_DIM] = result.astype(jnp.bfloat16)


VMEM = pl.BlockSpec(memory_space=pltpu.VMEM)
SMEM = pl.BlockSpec(memory_space=pltpu.SMEM)
HBM = pl.BlockSpec(memory_space=pltpu.HBM)


def call(kernel, out_shape, in_specs, scratch_shapes=(), **static):
    many = isinstance(out_shape, list)
    return pl.pallas_call(
        functools.partial(kernel, **static),
        out_shape=out_shape,
        in_specs=in_specs,
        out_specs=[VMEM] * len(out_shape) if many else VMEM,
        scratch_shapes=scratch_shapes,
        compiler_params=pltpu.CompilerParams(vmem_limit_bytes=VMEM_BYTES),
    )


def body(queries, root_keys, root_values, branch_keys, branch_values, branch_id, doc_len):
    shares = lax.axis_size("seq")
    row_dev, width = queries.shape
    rows = branch_id.shape[0]
    kv_local = root_keys.shape[1] // HEAD_DIM
    heads = kv_local * GROUP
    part = width // kv_local
    branch_dev, branch_len, _ = branch_keys.shape
    most_rows = 2 * row_dev // branch_dev
    slots = branch_dev * most_rows
    block = GROUP * row_dev
    f32 = functools.partial(jax.ShapeDtypeStruct, dtype=jnp.float32)
    bf16 = functools.partial(jax.ShapeDtypeStruct, dtype=jnp.bfloat16)
    scores = pltpu.VMEM((2, block, max(root_keys.shape[0], branch_len)), jnp.float32)
    some_rows = pltpu.VMEM((rows, part), jnp.bfloat16)
    result = [f32((kv_local, block, HEAD_DIM)), f32((row_dev, HEAD_DIM))]
    payload = bf16((heads * row_dev + row_dev // 2, HEAD_DIM))

    def swap(x, k):
        return lax.ppermute(x, "seq", [(i, i ^ k) for i in range(shares)])

    _, early, last, first, later = plan(shares)
    gathered = {}
    for k in early:
        gathered[k] = swap(queries, k)
    pieces_of_last = []
    for f in range(kv_local):
        piece = queries[:, f * part:(f + 1) * part]
        pieces_of_last.append(swap(piece, last))
    stored = (root_keys, root_values, branch_keys, branch_values)
    rk, rv, bk, bv, pick, bias, *mine = call(
        own,
        [bf16(x.shape) for x in stored] + [bf16((branch_dev, rows, most_rows)), f32((branch_dev, branch_len))] + result,
        [HBM] * 7,
        [scores, pltpu.VMEM((1, rows), jnp.int32), pltpu.VMEM((row_dev, width), jnp.bfloat16), pltpu.SMEM(doc_len.shape, jnp.int32), pltpu.SemaphoreType.DMA((7,))],
        kv_local=kv_local,
    )(*[pltpu.with_memory_space_constraint(x, pltpu.HBM) for x in (branch_id.reshape(1, rows), queries, root_keys, doc_len, *stored[1:])])
    ready = {0: mine}
    for k in early:
        ready[k] = call(root, result, [VMEM] * 3, [scores], kv_local=kv_local)(gathered[k], rk, rv)
    keys = [0] + early + [last]
    chunks = [queries] + [gathered[k] for k in early]
    branch_out, totals, sent = [], [], {first: []}
    for f in range(kv_local):
        partial, out, total = call(
            branch,
            [bf16((block + row_dev // 2, HEAD_DIM)), bf16((slots, part)), bf16((slots, 3 * HEAD_DIM))],
            [VMEM] * (6 + f + len(totals) + shares),
            [scores, some_rows],
            keys=keys,
            f=f,
            key=first,
            kv_local=kv_local,
        )(pick, bias, bk, bv, *ready[first], *branch_out, *totals, *chunks, pieces_of_last[f])
        branch_out.append(out)
        totals = [total]
        sent[first].append(partial)
    for k in later:
        if k in ready:
            partial = call(given, payload, [VMEM] * (4 + kv_local), key=k)(pick, *totals, *ready[k], *branch_out)
        else:
            partial = call(share, payload, [VMEM] * (4 + 2 * kv_local), [scores], key=k, kv_local=kv_local)(pick, *totals, rk, rv, *branch_out, *pieces_of_last)
        sent[k] = [partial]
    received, counts = [*sent[0]], [1]
    for k in [first] + later[:-1]:
        for partial in sent[k]:
            received.append(swap(partial, k))
        counts.append(len(sent[k]))
    return call(join, bf16((row_dev, width)), [VMEM] * len(received), heads=heads, counts=counts)(*received)


def plan(shares):
    order = list(range(1, shares))
    order = [shares // 2] + [k for k in order if k != shares // 2]
    return order, order[:-1], order[-1], order[0], [order[-1]] + order[1:-1] + [0]


def solution(mesh):
    rows = P(("parts", "seq"), "head")
    in_specs = (
        rows,
        rows,
        rows,
        P(("parts", "seq"), None, "head"),
        P(("parts", "seq"), None, "head"),
        P("parts", None),
        P("parts"),
    )

    return jax.shard_map(body, mesh=mesh, in_specs=in_specs, out_specs=rows, check_vma=False)
```

```python
import functools
import math

import jax
import jax.numpy as jnp
from jax import lax
from jax.experimental import pallas as pl
from jax.experimental.pallas import tpu as pltpu
from jax.sharding import PartitionSpec as P

QHEADS = 64
KVHEADS = 8
HEAD_DIM = 128
GROUP = QHEADS // KVHEADS
LOW = -1.0e30
SCALE = HEAD_DIM ** -0.5 * math.log2(math.e)
TILE = 256
VMEM_BYTES = 20 * 2 ** 20


def dot(a, b, dims=(((1,), (0,)), ((), ()))):
    return lax.dot_general(a, b, dims, preferred_element_type=jnp.float32)


def pieces(x):
    hi = x.astype(jnp.bfloat16)
    rest = x - hi.astype(jnp.float32)
    mid = rest.astype(jnp.bfloat16)
    low = (rest - mid.astype(jnp.float32)).astype(jnp.bfloat16)
    return hi, mid, low


def pipeline(blocks, score_ref):
    query, best = {}, {}

    def tiles(i):
        return [slice(at, at + TILE) for at in range(0, blocks[i][4], TILE)] if i < len(blocks) else []

    def score(i, at):
        if i not in query:
            query[i] = blocks[i][0]()
        s = dot(query[i], blocks[i][1](at), (((1,), (1,)), ((), ())))
        if blocks[i][3] is not None:
            s = s + blocks[i][3](at)
        score_ref[i % 2, :, at] = s
        for part in range(TILE // HEAD_DIM):
            t = s[:, part * HEAD_DIM:(part + 1) * HEAD_DIM]
            best[i] = jnp.maximum(best[i], t) if i in best else t

    for at in tiles(0):
        score(0, at)
    for i, (_, _, values, _, _, finish) in enumerate(blocks):
        peak = jnp.broadcast_to(jnp.max(best[i], axis=1, keepdims=True) * SCALE, best[i].shape)
        wide = jnp.concatenate([peak] * (TILE // HEAD_DIM), axis=1)
        ahead = tiles(i + 1)
        out = None
        for at in tiles(i):
            for later in ahead[:1]:
                score(i + 1, later)
            ahead = ahead[1:]
            w = jnp.exp2(score_ref[i % 2, :, at] * SCALE - wide).astype(jnp.bfloat16)
            part = dot(w, jnp.concatenate([values(at), jnp.ones((TILE, HEAD_DIM), jnp.bfloat16)], axis=1))
            out = part if out is None else out + part
        for later in ahead:
            score(i + 1, later)
        whole = out[:, HEAD_DIM:]
        finish(out[:, :HEAD_DIM] / whole, peak + jnp.log2(whole))


def stack_heads(chunk, first=0):
    return jnp.concatenate([chunk[:, (first + h) * HEAD_DIM:(first + h + 1) * HEAD_DIM] for h in range(GROUP)], axis=0)


def compact(levels):
    rows = next(iter(levels.values())).shape[0] // GROUP
    lane = lax.broadcasted_iota(jnp.int32, (rows, HEAD_DIM), 1)
    result = jnp.zeros((rows, HEAD_DIM), jnp.float32)
    for f, level in levels.items():
        for h in range(GROUP):
            result = jnp.where(lane == f * GROUP + h, level[h * rows:(h + 1) * rows, :], result)
    return result


def spread(stat, h, rows):
    return jnp.broadcast_to(stat[:, h:h + 1], (rows, HEAD_DIM))


def roots(query, rk_ref, rv_ref, heads, finish):
    outputs, levels = {}, {}

    def block(f):
        cut = slice(f * HEAD_DIM, (f + 1) * HEAD_DIM)

        def done(output, level):
            outputs[f], levels[f] = output, level
            if len(levels) == len(heads):
                finish(outputs, compact(levels))

        return (lambda: query(f), lambda at: rk_ref[at, cut], lambda at: rv_ref[at, cut], None, rk_ref.shape[0], done)

    return [block(f) for f in heads]


def store(out_ref, level_ref):
    def finish(outputs, level):
        for f, output in outputs.items():
            out_ref[f] = output
        level_ref[...] = level

    return finish


def own(*rest, kv_local):
    sources, rest = rest[:7], rest[7:]
    rk_ref, rv_ref, bk_ref, bv_ref, pick_ref, bias_ref, out_ref, level_ref = rest[:8]
    cut_refs, (score_ref, id_ref, q_ref, doc_ref, arrived) = rest[8:8 + kv_local], rest[8 + kv_local:]
    loads = [pltpu.make_async_copy(source, target, arrived.at[n]) for n, (source, target) in enumerate(zip(sources, (doc_ref, id_ref, q_ref, rk_ref, rv_ref, bk_ref, bv_ref)))]
    for load in loads:
        load.start()
    branch_dev, rows, most_rows = pick_ref.shape
    me = lax.axis_index("seq").astype(jnp.int32)
    loads[0].wait()
    slot = lax.broadcasted_iota(jnp.int32, (1, bias_ref.shape[1]), 1)
    for b in range(branch_dev):
        bias_ref[b:b + 1, :] = jnp.where(slot < doc_ref[me * branch_dev + b], 0.0, LOW)
    loads[1].wait()
    ids = id_ref[...]
    before = jnp.where(lax.broadcasted_iota(jnp.int32, (rows, rows), 0) < lax.broadcasted_iota(jnp.int32, (rows, rows), 1), 1.0, 0.0).astype(jnp.bfloat16)
    slot = lax.broadcasted_iota(jnp.int32, (most_rows, rows), 0).astype(jnp.float32)
    unit = jnp.where(lax.broadcasted_iota(jnp.int32, (most_rows, most_rows), 0) == lax.broadcasted_iota(jnp.int32, (most_rows, most_rows), 1), 1.0, 0.0).astype(jnp.bfloat16)
    for b in range(branch_dev):
        named = jnp.broadcast_to(jnp.where(ids == me * branch_dev + b, 1.0, 0.0), (most_rows, rows))
        rank = dot(named.astype(jnp.bfloat16), before)
        chosen = jnp.where((rank == slot) & (named > 0.0), 1.0, 0.0).astype(jnp.bfloat16)
        pick_ref[b] = dot(chosen, unit, (((0,), (0,)), ((), ()))).astype(jnp.bfloat16)
    loads[2].wait()
    part = q_ref.shape[1] // kv_local
    for f in range(kv_local):
        cut_refs[f][...] = q_ref[:, f * part:(f + 1) * part]
    for load in loads[3:5]:
        load.wait()
    pipeline(roots(lambda f: stack_heads(q_ref, f * GROUP), rk_ref, rv_ref, range(kv_local), store(out_ref, level_ref)), score_ref)
    for load in loads[5:]:
        load.wait()


def root(q_ref, rk_ref, rv_ref, out_ref, level_ref, score_ref, *, kv_local):
    pipeline(roots(lambda f: stack_heads(q_ref, f * GROUP), rk_ref, rv_ref, range(kv_local), store(out_ref, level_ref)), score_ref)


def source_of(sources):
    me = lax.axis_index("seq").astype(jnp.int32)
    result = jnp.int32(sources[0])
    for device in range(1, len(sources)):
        result = jnp.where(me == device, sources[device], result)
    return result


def picks(pick_ref, sources, row_dev):
    source = source_of(sources)
    at = pl.ds(pl.multiple_of(source * row_dev, row_dev), row_dev)
    return [pick_ref[b, at, :] for b in range(pick_ref.shape[0])]


def merge(share_ref, pick, outputs, level, branch_refs, b_level):
    row_dev = level.shape[0]
    pick = jnp.concatenate(pick, axis=1)
    has = jnp.sum(pick.astype(jnp.float32), axis=1, keepdims=True) > 0.0
    found = dot(pick, b_level)
    b_level = jnp.where(has, found[:, :HEAD_DIM] + found[:, HEAD_DIM:2 * HEAD_DIM] + found[:, 2 * HEAD_DIM:], LOW)
    top = jnp.maximum(level, b_level)
    ours, theirs = jnp.exp2(level - top), jnp.exp2(b_level - top)
    both = ours + theirs
    ours, theirs = ours / both, theirs / both
    for n, (f, output) in enumerate(outputs.items()):
        b_out = dot(pick, branch_refs[f][...])
        for g in range(GROUP):
            h = f * GROUP + g
            at = (n * GROUP + g) * row_dev
            ahead = output[g * row_dev:(g + 1) * row_dev, :] * spread(ours, h, row_dev)
            share_ref[at:at + row_dev, :] = (ahead + b_out[:, g * HEAD_DIM:(g + 1) * HEAD_DIM] * spread(theirs, h, row_dev)).astype(jnp.bfloat16)
    lane = lax.broadcasted_iota(jnp.int32, (row_dev, HEAD_DIM), 1)
    here = functools.reduce(jnp.logical_or, [(lane >= f * GROUP) & (lane < (f + 1) * GROUP) for f in outputs])
    stat = jnp.where(here, top + jnp.log2(both), 0.0)
    heads = len(branch_refs) * GROUP
    stat = stat + pltpu.roll(stat, heads, 1) + pltpu.roll(stat, 2 * heads, 1)
    hi, mid, low = [piece.astype(jnp.float32) for piece in pieces(stat)]
    packed = jnp.where(lane < heads, hi, jnp.where(lane < 2 * heads, mid, low))
    half = row_dev // 2
    share_ref[len(outputs) * GROUP * row_dev:, :] = (packed[:half] + pltpu.roll(packed[half:], HEAD_DIM // 2, 1)).astype(jnp.bfloat16)


def branch_blocks(pick_ref, bias_ref, bk_ref, bv_ref, q_refs, rows_ref, branch_ref, keys, f, finish):
    row_dev = q_refs[0].shape[0]
    branch_dev, _, most_rows = pick_ref.shape
    part = rows_ref.shape[1]
    cut = slice(f * HEAD_DIM, (f + 1) * HEAD_DIM)
    for sources, q_ref in zip(keys, q_refs):
        at = pl.ds(pl.multiple_of(source_of(sources) * row_dev, row_dev), row_dev)
        rows_ref[at, :] = q_ref[...] if q_ref is q_refs[-1] else q_ref[:, f * part:(f + 1) * part]
    named = jnp.concatenate([pick_ref[b] for b in range(branch_dev)], axis=1)
    picked = dot(named, rows_ref[...], (((0,), (0,)), ((), ()))).astype(jnp.bfloat16)
    levels = []

    def block(b):
        def done(output, level):
            for h in range(GROUP):
                branch_ref[b * most_rows:(b + 1) * most_rows, h * HEAD_DIM:(h + 1) * HEAD_DIM] = output[h * most_rows:(h + 1) * most_rows].astype(jnp.bfloat16)
            levels.append(compact({f: level}))
            if len(levels) == branch_dev:
                finish(jnp.concatenate(levels, axis=0))

        return (lambda: stack_heads(picked[b * most_rows:(b + 1) * most_rows]), lambda at: bk_ref[b, at, cut], lambda at: bv_ref[b, at, cut], lambda at: bias_ref[b:b + 1, at], bk_ref.shape[1], done)

    return [block(b) for b in range(branch_dev)]


def branch(pick_ref, bias_ref, bk_ref, bv_ref, *rest, keys, f, key, kv_local):
    ends = f == kv_local - 1
    branch_refs, rest = rest[:f], rest[f:]
    total_refs, rest = rest[:min(f, 1)], rest[min(f, 1):]
    q_refs, rest = rest[:len(keys)], rest[len(keys):]
    given_refs, rest = (rest[:2], rest[2:]) if ends else ((), rest)
    branch_ref, total_ref, *share_refs, score_ref, rows_ref = rest

    def finish(level):
        total = jnp.concatenate(pieces(level), axis=1)
        for ref in total_refs:
            total = total + ref[...]
        total_ref[...] = total

    pipeline(branch_blocks(pick_ref, bias_ref, bk_ref, bv_ref, q_refs, rows_ref, branch_ref, keys, f, finish), score_ref)
    if ends:
        out_ref, level_ref = given_refs
        merge(share_refs[0], picks(pick_ref, key, level_ref.shape[0]), {g: out_ref[g] for g in range(kv_local)}, level_ref[...], [*branch_refs, branch_ref], total_ref[...])


def share(pick_ref, b_level_ref, rk_ref, rv_ref, *rest, key, kv_local):
    branch_refs, q_refs, share_ref, score_ref = rest[:kv_local], rest[kv_local:2 * kv_local], rest[-2], rest[-1]

    def finish(outputs, level):
        merge(share_ref, picks(pick_ref, key, level.shape[0]), outputs, level, branch_refs, b_level_ref[...])

    pipeline(roots(lambda f: stack_heads(q_refs[f]), rk_ref, rv_ref, range(kv_local), finish), score_ref)


def given(pick_ref, b_level_ref, out_ref, level_ref, *rest, key):
    branch_refs, share_ref = rest[:-1], rest[-1]
    merge(share_ref, picks(pick_ref, key, level_ref.shape[0]), {f: out_ref[f] for f in range(len(branch_refs))}, level_ref[...], branch_refs, b_level_ref[...])


def join(*refs, heads):
    share_refs, out_ref = refs[:-1], refs[-1]
    row_dev = out_ref.shape[0]
    half = row_dev // 2
    levels = []
    for ref in share_refs:
        s = ref[heads * row_dev:, :].astype(jnp.float32)
        levels.append(s + pltpu.roll(s, HEAD_DIM - heads, 1) + pltpu.roll(s, HEAD_DIM - 2 * heads, 1))
    top = functools.reduce(jnp.maximum, levels)
    parts = [jnp.exp2(x - top) for x in levels]
    whole = functools.reduce(jnp.add, parts)
    parts = [x / whole for x in parts]
    for h in range(heads):
        result = None
        for ref, part in zip(share_refs, parts):
            factor = jnp.concatenate([spread(part, h, half), spread(part, HEAD_DIM // 2 + h, half)], axis=0)
            term = ref[h * row_dev:(h + 1) * row_dev, :].astype(jnp.float32) * factor
            result = term if result is None else result + term
        out_ref[:, h * HEAD_DIM:(h + 1) * HEAD_DIM] = result.astype(jnp.bfloat16)


VMEM = pl.BlockSpec(memory_space=pltpu.VMEM)
SMEM = pl.BlockSpec(memory_space=pltpu.SMEM)
HBM = pl.BlockSpec(memory_space=pltpu.HBM)


def call(kernel, out_shape, in_specs, scratch_shapes=(), **static):
    many = isinstance(out_shape, list)
    return pl.pallas_call(
        functools.partial(kernel, **static),
        out_shape=out_shape,
        in_specs=in_specs,
        out_specs=[VMEM] * len(out_shape) if many else VMEM,
        scratch_shapes=scratch_shapes,
        compiler_params=pltpu.CompilerParams(vmem_limit_bytes=VMEM_BYTES),
    )


def body(queries, root_keys, root_values, branch_keys, branch_values, branch_id, doc_len):
    shares = lax.axis_size("seq")
    row_dev, width = queries.shape
    rows = branch_id.shape[0]
    kv_local = root_keys.shape[1] // HEAD_DIM
    heads = kv_local * GROUP
    part = width // kv_local
    branch_dev, branch_len, _ = branch_keys.shape
    most_rows = 2 * row_dev // branch_dev
    slots = branch_dev * most_rows
    block = GROUP * row_dev
    f32 = functools.partial(jax.ShapeDtypeStruct, dtype=jnp.float32)
    bf16 = functools.partial(jax.ShapeDtypeStruct, dtype=jnp.bfloat16)
    scores = pltpu.VMEM((2, block, max(root_keys.shape[0], branch_len)), jnp.float32)
    some_rows = pltpu.VMEM((rows, part), jnp.bfloat16)
    result = [f32((kv_local, block, HEAD_DIM)), f32((row_dev, HEAD_DIM))]
    payload = bf16((heads * row_dev + row_dev // 2, HEAD_DIM))

    def move(x, targets):
        return lax.ppermute(x, "seq", list(enumerate(targets)))

    rounds = plan(shares)
    back = [inverse(targets) for targets in rounds]
    early, last = range(len(rounds) - 1), len(rounds) - 1
    gathered = []
    for n in early:
        gathered.append(move(queries, rounds[n]))
    stored = (root_keys, root_values, branch_keys, branch_values)
    rk, rv, bk, bv, pick, bias, *mine = call(
        own,
        [bf16(x.shape) for x in stored] + [bf16((branch_dev, rows, most_rows)), f32((branch_dev, branch_len))] + result + [bf16((row_dev, part))] * kv_local,
        [HBM] * 7,
        [scores, pltpu.VMEM((1, rows), jnp.int32), pltpu.VMEM((row_dev, width), jnp.bfloat16), pltpu.SMEM(doc_len.shape, jnp.int32), pltpu.SemaphoreType.DMA((7,))],
        kv_local=kv_local,
    )(*[pltpu.with_memory_space_constraint(x, pltpu.HBM) for x in (doc_len, branch_id.reshape(1, rows), queries, *stored)])
    pieces_of_last = []
    for f in range(kv_local):
        pieces_of_last.append(move(mine[2 + f], rounds[last]))
    ready = []
    for n in early:
        ready.append(call(root, result, [VMEM] * 3, [scores], kv_local=kv_local)(gathered[n], rk, rv))
    keys = [tuple(range(shares))] + back
    branch_out, totals, sent = [], [], []
    for f in range(kv_local):
        ends = f == kv_local - 1
        out, total, *partial = call(
            branch,
            [bf16((slots, part)), bf16((slots, 3 * HEAD_DIM))] + [payload] * ends,
            [VMEM] * (4 + f + len(totals) + shares + 2 * ends),
            [scores, some_rows],
            keys=keys,
            f=f,
            key=back[0],
            kv_local=kv_local,
        )(pick, bias, bk, bv, *branch_out, *totals, queries, *gathered, pieces_of_last[f], *(ready[0] if ends else ()))
        branch_out.append(out)
        totals = [total]
    sent = partial
    for n in early[1:]:
        sent.append(call(given, payload, [VMEM] * (4 + kv_local), key=back[n])(pick, *totals, *ready[n], *branch_out))
    sent.append(call(share, payload, [VMEM] * (4 + 2 * kv_local), [scores], key=back[last], kv_local=kv_local)(pick, *totals, rk, rv, *branch_out, *pieces_of_last))
    received = [call(given, payload, [VMEM] * (4 + kv_local), key=keys[0])(pick, *totals, *mine[:2], *branch_out)]
    for n, partial in enumerate(sent):
        received.append(move(partial, back[n]))
    return call(join, bf16((row_dev, width)), [VMEM] * shares, heads=heads)(*received)


def inverse(targets):
    return tuple(targets.index(device) for device in range(len(targets)))


def plan(shares):
    if shares == 4:
        return [(2, 0, 3, 1), (1, 3, 0, 2), (3, 2, 1, 0)]
    return [tuple(device ^ k for device in range(shares)) for k in range(1, shares)]


def solution(mesh):
    rows = P(("parts", "seq"), "head")
    in_specs = (
        rows,
        rows,
        rows,
        P(("parts", "seq"), None, "head"),
        P(("parts", "seq"), None, "head"),
        P("parts", None),
        P("parts"),
    )

    return jax.shard_map(body, mesh=mesh, in_specs=in_specs, out_specs=rows, check_vma=False)
```

```python
import functools
import math

import jax
import jax.numpy as jnp
from jax import lax
from jax.experimental import pallas as pl
from jax.experimental.pallas import tpu as pltpu
from jax.sharding import PartitionSpec as P

QHEADS = 64
KVHEADS = 8
HEAD_DIM = 128
GROUP = QHEADS // KVHEADS
LOW = -1.0e30
SCALE = HEAD_DIM ** -0.5 * math.log2(math.e)
TILE = 256
VMEM_BYTES = 20 * 2 ** 20


def dot(a, b, dims=(((1,), (0,)), ((), ()))):
    return lax.dot_general(a, b, dims, preferred_element_type=jnp.float32)


def pieces(x):
    hi = x.astype(jnp.bfloat16)
    rest = x - hi.astype(jnp.float32)
    mid = rest.astype(jnp.bfloat16)
    low = (rest - mid.astype(jnp.float32)).astype(jnp.bfloat16)
    return hi, mid, low


def pipeline(blocks, score_ref):
    query, best = {}, {}

    def tiles(i):
        return [slice(at, at + TILE) for at in range(0, blocks[i][4], TILE)] if i < len(blocks) else []

    def score(i, at):
        if i not in query:
            query[i] = blocks[i][0]()
        s = dot(query[i], blocks[i][1](at), (((1,), (1,)), ((), ())))
        if blocks[i][3] is not None:
            s = s + blocks[i][3](at)
        score_ref[i % 2, :, at] = s
        for part in range(TILE // HEAD_DIM):
            t = s[:, part * HEAD_DIM:(part + 1) * HEAD_DIM]
            best[i] = jnp.maximum(best[i], t) if i in best else t

    for at in tiles(0):
        score(0, at)
    for i, (_, _, values, _, _, finish) in enumerate(blocks):
        peak = jnp.broadcast_to(jnp.max(best[i], axis=1, keepdims=True) * SCALE, best[i].shape)
        wide = jnp.concatenate([peak] * (TILE // HEAD_DIM), axis=1)
        ahead = tiles(i + 1)
        out = None
        for at in tiles(i):
            for later in ahead[:1]:
                score(i + 1, later)
            ahead = ahead[1:]
            w = jnp.exp2(score_ref[i % 2, :, at] * SCALE - wide).astype(jnp.bfloat16)
            part = dot(w, jnp.concatenate([values(at), jnp.ones((TILE, HEAD_DIM), jnp.bfloat16)], axis=1))
            out = part if out is None else out + part
        for later in ahead:
            score(i + 1, later)
        whole = out[:, HEAD_DIM:]
        finish(out[:, :HEAD_DIM] / whole, peak + jnp.log2(whole))


def stack_heads(chunk, first=0):
    return jnp.concatenate([chunk[:, (first + h) * HEAD_DIM:(first + h + 1) * HEAD_DIM] for h in range(GROUP)], axis=0)


def compact(levels):
    rows = next(iter(levels.values())).shape[0] // GROUP
    lane = lax.broadcasted_iota(jnp.int32, (rows, HEAD_DIM), 1)
    result = jnp.zeros((rows, HEAD_DIM), jnp.float32)
    for f, level in levels.items():
        for h in range(GROUP):
            result = jnp.where(lane == f * GROUP + h, level[h * rows:(h + 1) * rows, :], result)
    return result


def spread(stat, h, rows):
    return jnp.broadcast_to(stat[:, h:h + 1], (rows, HEAD_DIM))


def roots(query, rk_ref, rv_ref, heads, finish):
    outputs, levels = {}, {}

    def block(f):
        cut = slice(f * HEAD_DIM, (f + 1) * HEAD_DIM)

        def done(output, level):
            outputs[f], levels[f] = output, level
            if len(levels) == len(heads):
                finish(outputs, compact(levels))

        return (lambda: query(f), lambda at: rk_ref[at, cut], lambda at: rv_ref[at, cut], None, rk_ref.shape[0], done)

    return [block(f) for f in heads]


def store(out_ref, level_ref):
    def finish(outputs, level):
        for f, output in outputs.items():
            out_ref[f] = output
        level_ref[...] = level

    return finish


def own(doc_hbm, id_hbm, rk_hbm, rv_hbm, bk_hbm, rk_ref, rv_ref, bk_ref, pick_ref, bias_ref, id_ref, doc_ref, arrived):
    loads = [pltpu.make_async_copy(source, target, arrived.at[n]) for n, (source, target) in enumerate(zip((doc_hbm, id_hbm, rk_hbm, rv_hbm, bk_hbm), (doc_ref, id_ref, rk_ref, rv_ref, bk_ref)))]
    for load in loads:
        load.start()
    branch_dev, rows, most_rows = pick_ref.shape
    me = lax.axis_index("seq").astype(jnp.int32)
    loads[0].wait()
    slot = lax.broadcasted_iota(jnp.int32, (1, bias_ref.shape[1]), 1)
    for b in range(branch_dev):
        bias_ref[b:b + 1, :] = jnp.where(slot < doc_ref[me * branch_dev + b], 0.0, LOW)
    loads[1].wait()
    ids = id_ref[...]
    before = jnp.where(lax.broadcasted_iota(jnp.int32, (rows, rows), 0) < lax.broadcasted_iota(jnp.int32, (rows, rows), 1), 1.0, 0.0).astype(jnp.bfloat16)
    slot = lax.broadcasted_iota(jnp.int32, (most_rows, rows), 0).astype(jnp.float32)
    unit = jnp.where(lax.broadcasted_iota(jnp.int32, (most_rows, most_rows), 0) == lax.broadcasted_iota(jnp.int32, (most_rows, most_rows), 1), 1.0, 0.0).astype(jnp.bfloat16)
    for b in range(branch_dev):
        named = jnp.broadcast_to(jnp.where(ids == me * branch_dev + b, 1.0, 0.0), (most_rows, rows))
        rank = dot(named.astype(jnp.bfloat16), before)
        chosen = jnp.where((rank == slot) & (named > 0.0), 1.0, 0.0).astype(jnp.bfloat16)
        pick_ref[b] = dot(chosen, unit, (((0,), (0,)), ((), ()))).astype(jnp.bfloat16)
    for load in loads[2:]:
        load.wait()


def root_load(q_ref, rk_ref, rv_ref, bv_hbm, out_ref, level_ref, bv_ref, score_ref, arrived, *, kv_local):
    load = pltpu.make_async_copy(bv_hbm, bv_ref, arrived)
    load.start()
    root(q_ref, rk_ref, rv_ref, out_ref, level_ref, score_ref, kv_local=kv_local)
    load.wait()


def root(q_ref, rk_ref, rv_ref, out_ref, level_ref, score_ref, *, kv_local):
    pipeline(roots(lambda f: stack_heads(q_ref, f * GROUP), rk_ref, rv_ref, range(kv_local), store(out_ref, level_ref)), score_ref)


def source_of(sources):
    me = lax.axis_index("seq").astype(jnp.int32)
    result = jnp.int32(sources[0])
    for device in range(1, len(sources)):
        result = jnp.where(me == device, sources[device], result)
    return result


def picks(pick_ref, sources, row_dev):
    source = source_of(sources)
    at = pl.ds(pl.multiple_of(source * row_dev, row_dev), row_dev)
    return [pick_ref[b, at, :] for b in range(pick_ref.shape[0])]


def merge(share_ref, pick, outputs, level, branch_ref, b_level):
    row_dev = level.shape[0]
    heads = len(outputs) * GROUP
    pick = jnp.concatenate(pick, axis=1)
    has = jnp.sum(pick.astype(jnp.float32), axis=1, keepdims=True) > 0.0
    found = dot(pick, b_level)
    b_level = jnp.where(has, found[:, :HEAD_DIM] + found[:, HEAD_DIM:2 * HEAD_DIM] + found[:, 2 * HEAD_DIM:], LOW)
    top = jnp.maximum(level, b_level)
    ours, theirs = jnp.exp2(level - top), jnp.exp2(b_level - top)
    both = ours + theirs
    ours, theirs = ours / both, theirs / both
    b_out = dot(pick, branch_ref[...])
    for f, output in enumerate(outputs):
        for g in range(GROUP):
            h = f * GROUP + g
            ahead = output[g * row_dev:(g + 1) * row_dev, :] * spread(ours, h, row_dev)
            share_ref[h * row_dev:(h + 1) * row_dev, :] = (ahead + b_out[:, h * HEAD_DIM:(h + 1) * HEAD_DIM] * spread(theirs, h, row_dev)).astype(jnp.bfloat16)
    write_level(share_ref, top + jnp.log2(both), heads)


def write_level(share_ref, level, heads):
    row_dev = level.shape[0]
    lane = lax.broadcasted_iota(jnp.int32, (row_dev, HEAD_DIM), 1)
    stat = jnp.where(lane < heads, level, 0.0)
    stat = stat + pltpu.roll(stat, heads, 1) + pltpu.roll(stat, 2 * heads, 1)
    hi, mid, low = [piece.astype(jnp.float32) for piece in pieces(stat)]
    packed = jnp.where(lane < heads, hi, jnp.where(lane < 2 * heads, mid, low))
    half = row_dev // 2
    share_ref[heads * row_dev:, :] = (packed[:half] + pltpu.roll(packed[half:], HEAD_DIM // 2, 1)).astype(jnp.bfloat16)


def branch(pick_ref, bias_ref, bk_ref, bv_ref, out_ref, level_ref, *rest, keys, direct, kv_local):
    q_refs, last_refs, rest = rest[:len(keys) - 1], rest[len(keys) - 1:-6], rest[-6:]
    share_ref, branch_ref, total_ref, last_ref, score_ref, rows_ref = rest
    row_dev, width = q_refs[0].shape
    branch_dev, _, most_rows = pick_ref.shape
    part = width // kv_local
    last = last_refs[0][...]
    if len(last_refs) > 1:
        last = jnp.where(source_of(direct) == 1, last, last_refs[1][...])
    last_ref[...] = last
    for sources, q_ref in zip(keys, [*q_refs, last_ref]):
        at = pl.ds(pl.multiple_of(source_of(sources) * row_dev, row_dev), row_dev)
        rows_ref[at, :] = q_ref[...]
    named = jnp.concatenate([pick_ref[b] for b in range(branch_dev)], axis=1)
    picked = dot(named, rows_ref[...], (((0,), (0,)), ((), ()))).astype(jnp.bfloat16)
    levels = [{} for _ in range(branch_dev)]

    def block(b, f):
        cut = slice(f * HEAD_DIM, (f + 1) * HEAD_DIM)

        def done(output, level):
            for h in range(GROUP):
                at = slice(f * part + h * HEAD_DIM, f * part + (h + 1) * HEAD_DIM)
                branch_ref[b * most_rows:(b + 1) * most_rows, at] = output[h * most_rows:(h + 1) * most_rows].astype(jnp.bfloat16)
            levels[b][f] = level

        return (lambda: stack_heads(picked[b * most_rows:(b + 1) * most_rows], f * GROUP), lambda at: bk_ref[b, at, cut], lambda at: bv_ref[b, at, cut], lambda at: bias_ref[b:b + 1, at], bk_ref.shape[1], done)

    pipeline([block(b, f) for b in range(branch_dev) for f in range(kv_local)], score_ref)
    total_ref[...] = jnp.concatenate(pieces(jnp.concatenate([compact(level) for level in levels], axis=0)), axis=1)
    merge(share_ref, picks(pick_ref, keys[1], row_dev), [out_ref[f] for f in range(kv_local)], level_ref[...], branch_ref, total_ref[...])


def share(pick_ref, b_level_ref, rk_ref, rv_ref, branch_ref, q_ref, share_ref, score_ref, *, key, kv_local):
    def finish(outputs, level):
        merge(share_ref, picks(pick_ref, key, level.shape[0]), list(outputs.values()), level, branch_ref, b_level_ref[...])

    pipeline(roots(lambda f: stack_heads(q_ref, f * GROUP), rk_ref, rv_ref, range(kv_local), finish), score_ref)


def given(pick_ref, b_level_ref, out_ref, level_ref, branch_ref, share_ref, *, key):
    merge(share_ref, picks(pick_ref, key, level_ref.shape[0]), [out_ref[f] for f in range(out_ref.shape[0])], level_ref[...], branch_ref, b_level_ref[...])


def join(*refs, heads):
    share_refs, out_ref = refs[:-1], refs[-1]
    row_dev = out_ref.shape[0]
    half = row_dev // 2
    levels = []
    for ref in share_refs:
        s = ref[heads * row_dev:, :].astype(jnp.float32)
        levels.append(s + pltpu.roll(s, HEAD_DIM - heads, 1) + pltpu.roll(s, HEAD_DIM - 2 * heads, 1))
    top = functools.reduce(jnp.maximum, levels)
    parts = [jnp.exp2(x - top) for x in levels]
    whole = functools.reduce(jnp.add, parts)
    parts = [x / whole for x in parts]
    for h in range(heads):
        result = None
        for ref, part in zip(share_refs, parts):
            factor = jnp.concatenate([spread(part, h, half), spread(part, HEAD_DIM // 2 + h, half)], axis=0)
            term = ref[h * row_dev:(h + 1) * row_dev, :].astype(jnp.float32) * factor
            result = term if result is None else result + term
        out_ref[:, h * HEAD_DIM:(h + 1) * HEAD_DIM] = result.astype(jnp.bfloat16)


VMEM = pl.BlockSpec(memory_space=pltpu.VMEM)
SMEM = pl.BlockSpec(memory_space=pltpu.SMEM)
HBM = pl.BlockSpec(memory_space=pltpu.HBM)


def call(kernel, out_shape, in_specs, scratch_shapes=(), **static):
    many = isinstance(out_shape, list)
    return pl.pallas_call(
        functools.partial(kernel, **static),
        out_shape=out_shape,
        in_specs=in_specs,
        out_specs=[VMEM] * len(out_shape) if many else VMEM,
        scratch_shapes=scratch_shapes,
        compiler_params=pltpu.CompilerParams(vmem_limit_bytes=VMEM_BYTES),
    )


def body(queries, root_keys, root_values, branch_keys, branch_values, branch_id, doc_len):
    shares = lax.axis_size("seq")
    row_dev, width = queries.shape
    rows = branch_id.shape[0]
    kv_local = root_keys.shape[1] // HEAD_DIM
    heads = kv_local * GROUP
    part = width // kv_local
    branch_dev, branch_len, _ = branch_keys.shape
    most_rows = 2 * row_dev // branch_dev
    slots = branch_dev * most_rows
    block = GROUP * row_dev
    f32 = functools.partial(jax.ShapeDtypeStruct, dtype=jnp.float32)
    bf16 = functools.partial(jax.ShapeDtypeStruct, dtype=jnp.bfloat16)
    scores = pltpu.VMEM((2, block, max(root_keys.shape[0], branch_len)), jnp.float32)
    some_rows = pltpu.VMEM((rows, part), jnp.bfloat16)
    result = [f32((kv_local, block, HEAD_DIM)), f32((row_dev, HEAD_DIM))]
    payload = bf16((heads * row_dev + row_dev // 2, HEAD_DIM))

    def move(x, targets):
        return lax.ppermute(x, "seq", [(i, target) for i, target in enumerate(targets) if target is not None])

    rounds, relay = plan(shares)
    back = [inverse(targets) for targets in rounds]
    early, last = range(len(rounds) - 1), len(rounds) - 1
    gathered = []
    for n in early:
        gathered.append(move(queries, rounds[n]))
    at_last = [move(queries, relay[0] if relay else rounds[last])]
    if relay:
        at_last.append(move(gathered[0], relay[1]))
    in_hbm = [pltpu.with_memory_space_constraint(x, pltpu.HBM) for x in (doc_len, branch_id.reshape(1, rows), root_keys, root_values, branch_keys, branch_values)]
    rk, rv, bk, pick, bias = call(
        own,
        [bf16(x.shape) for x in (root_keys, root_values, branch_keys)] + [bf16((branch_dev, rows, most_rows)), f32((branch_dev, branch_len))],
        [HBM] * 5,
        [pltpu.VMEM((1, rows), jnp.int32), pltpu.SMEM(doc_len.shape, jnp.int32), pltpu.SemaphoreType.DMA((5,))],
    )(*in_hbm[:5])
    ready = []
    for n in early:
        if n == 0:
            *first, bv = call(
                root_load, result + [bf16(branch_values.shape)], [VMEM] * 3 + [HBM], [scores, pltpu.SemaphoreType.DMA(())], kv_local=kv_local
            )(gathered[n], rk, rv, in_hbm[5])
            ready.append(first)
        else:
            ready.append(call(root, result, [VMEM] * 3, [scores], kv_local=kv_local)(gathered[n], rk, rv))
    keys = [tuple(range(shares))] + back
    partial, out, total, rest = call(
        branch,
        [payload, bf16((slots, width)), bf16((slots, 3 * HEAD_DIM)), bf16((row_dev, width))],
        [VMEM] * (5 + shares + len(at_last)),
        [scores, pltpu.VMEM((rows, width), jnp.bfloat16)],
        keys=keys,
        direct=tuple(int(a == b) for a, b in zip(inverse(relay[0]), back[last])) if relay else None,
        kv_local=kv_local,
    )(pick, bias, bk, bv, *ready[0], queries, *gathered, *at_last)
    sent = [partial]
    for n in early[1:]:
        sent.append(call(given, payload, [VMEM] * 5, key=back[n])(pick, total, *ready[n], out))
    sent.append(call(share, payload, [VMEM] * 6, [scores], key=back[last], kv_local=kv_local)(pick, total, rk, rv, out, rest))
    received = [call(share, payload, [VMEM] * 6, [scores], key=keys[0], kv_local=kv_local)(pick, total, rk, rv, out, queries)]
    for n, partial in enumerate(sent):
        received.append(move(partial, back[n]))
    return call(join, bf16((row_dev, width)), [VMEM] * shares, heads=heads)(*received)


def inverse(targets):
    return tuple(targets.index(device) if device in targets else None for device in range(len(targets)))


def plan(shares):
    if shares == 4:
        return [(2, 0, 3, 1), (1, 3, 0, 2), (3, 2, 1, 0)], [(0, 2, 1, 3), (1, 0, 3, 2)]
    return [tuple(device ^ k for device in range(shares)) for k in range(1, shares)], None


def solution(mesh):
    rows = P(("parts", "seq"), "head")
    in_specs = (
        rows,
        rows,
        rows,
        P(("parts", "seq"), None, "head"),
        P(("parts", "seq"), None, "head"),
        P("parts", None),
        P("parts"),
    )

    return jax.shard_map(body, mesh=mesh, in_specs=in_specs, out_specs=rows, check_vma=False)
```

```python
import functools
import math

import jax
import jax.numpy as jnp
from jax import lax
from jax.experimental import pallas as pl
from jax.experimental.pallas import tpu as pltpu
from jax.sharding import PartitionSpec as P

QHEADS = 64
KVHEADS = 8
HEAD_DIM = 128
GROUP = QHEADS // KVHEADS
LOW = -1.0e30
SCALE = HEAD_DIM ** -0.5 * math.log2(math.e)
TILE = 512
VMEM_BYTES = 20 * 2 ** 20


def dot(a, b, dims=(((1,), (0,)), ((), ()))):
    return lax.dot_general(a, b, dims, preferred_element_type=jnp.float32)


def pieces(x):
    hi = x.astype(jnp.bfloat16)
    rest = x - hi.astype(jnp.float32)
    mid = rest.astype(jnp.bfloat16)
    low = (rest - mid.astype(jnp.float32)).astype(jnp.bfloat16)
    return hi, mid, low


def pipeline(blocks, score_ref):
    query, best = {}, {}

    def tiles(i):
        return [slice(at, at + TILE) for at in range(0, blocks[i][4], TILE)] if i < len(blocks) else []

    def score(i, at):
        if i not in query:
            query[i] = blocks[i][0]()
        s = dot(query[i], blocks[i][1](at), (((1,), (1,)), ((), ())))
        if blocks[i][3] is not None:
            s = s + blocks[i][3](at)
        score_ref[i % 2, :, at] = s
        for part in range(TILE // HEAD_DIM):
            t = s[:, part * HEAD_DIM:(part + 1) * HEAD_DIM]
            best[i] = jnp.maximum(best[i], t) if i in best else t

    for at in tiles(0):
        score(0, at)
    for i, (_, _, values, _, _, finish) in enumerate(blocks):
        peak = jnp.broadcast_to(jnp.max(best[i], axis=1, keepdims=True) * SCALE, best[i].shape)
        wide = jnp.concatenate([peak] * (TILE // HEAD_DIM), axis=1)
        ahead = tiles(i + 1)
        out = None
        for at in tiles(i):
            for later in ahead[:1]:
                score(i + 1, later)
            ahead = ahead[1:]
            w = jnp.exp2(score_ref[i % 2, :, at] * SCALE - wide).astype(jnp.bfloat16)
            part = dot(w, jnp.concatenate([values(at), jnp.ones((TILE, HEAD_DIM), jnp.bfloat16)], axis=1))
            out = part if out is None else out + part
        for later in ahead:
            score(i + 1, later)
        whole = out[:, HEAD_DIM:]
        finish(out[:, :HEAD_DIM] / whole, peak + jnp.log2(whole))


def stack_heads(chunk, first=0):
    return jnp.concatenate([chunk[:, (first + h) * HEAD_DIM:(first + h + 1) * HEAD_DIM] for h in range(GROUP)], axis=0)


def compact(levels):
    rows = next(iter(levels.values())).shape[0] // GROUP
    lane = lax.broadcasted_iota(jnp.int32, (rows, HEAD_DIM), 1)
    result = jnp.zeros((rows, HEAD_DIM), jnp.float32)
    for f, level in levels.items():
        for h in range(GROUP):
            result = jnp.where(lane == f * GROUP + h, level[h * rows:(h + 1) * rows, :], result)
    return result


def spread(stat, h, rows):
    return jnp.broadcast_to(stat[:, h:h + 1], (rows, HEAD_DIM))


def roots(query, rk_ref, rv_ref, heads, finish):
    outputs, levels = {}, {}

    def block(f):
        cut = slice(f * HEAD_DIM, (f + 1) * HEAD_DIM)

        def done(output, level):
            outputs[f], levels[f] = output, level
            if len(levels) == len(heads):
                finish(outputs, compact(levels))

        return (lambda: query(f), lambda at: rk_ref[at, cut], lambda at: rv_ref[at, cut], None, rk_ref.shape[0], done)

    return [block(f) for f in heads]


def store(out_ref, level_ref):
    def finish(outputs, level):
        for f, output in outputs.items():
            out_ref[f] = output
        level_ref[...] = level

    return finish


def own(doc_hbm, id_hbm, rk_hbm, rv_hbm, rk_ref, rv_ref, pick_ref, bias_ref, id_ref, doc_ref, arrived):
    loads = [pltpu.make_async_copy(source, target, arrived.at[n]) for n, (source, target) in enumerate(zip((doc_hbm, id_hbm, rk_hbm, rv_hbm), (doc_ref, id_ref, rk_ref, rv_ref)))]
    for load in loads:
        load.start()
    branch_dev, rows, most_rows = pick_ref.shape
    me = lax.axis_index("seq").astype(jnp.int32)
    loads[0].wait()
    slot = lax.broadcasted_iota(jnp.int32, (1, bias_ref.shape[1]), 1)
    for b in range(branch_dev):
        bias_ref[b:b + 1, :] = jnp.where(slot < doc_ref[me * branch_dev + b], 0.0, LOW)
    loads[1].wait()
    ids = id_ref[...]
    before = jnp.where(lax.broadcasted_iota(jnp.int32, (rows, rows), 0) < lax.broadcasted_iota(jnp.int32, (rows, rows), 1), 1.0, 0.0).astype(jnp.bfloat16)
    slot = lax.broadcasted_iota(jnp.int32, (most_rows, rows), 0).astype(jnp.float32)
    unit = jnp.where(lax.broadcasted_iota(jnp.int32, (most_rows, most_rows), 0) == lax.broadcasted_iota(jnp.int32, (most_rows, most_rows), 1), 1.0, 0.0).astype(jnp.bfloat16)
    for b in range(branch_dev):
        named = jnp.broadcast_to(jnp.where(ids == me * branch_dev + b, 1.0, 0.0), (most_rows, rows))
        rank = dot(named.astype(jnp.bfloat16), before)
        chosen = jnp.where((rank == slot) & (named > 0.0), 1.0, 0.0).astype(jnp.bfloat16)
        pick_ref[b] = dot(chosen, unit, (((0,), (0,)), ((), ()))).astype(jnp.bfloat16)
    for load in loads[2:]:
        load.wait()


def root_load(q_ref, rk_ref, rv_ref, stored_hbm, out_ref, level_ref, stored_ref, score_ref, arrived, *, kv_local):
    load = pltpu.make_async_copy(stored_hbm, stored_ref, arrived)
    load.start()
    root(q_ref, rk_ref, rv_ref, out_ref, level_ref, score_ref, kv_local=kv_local)
    load.wait()


def root(q_ref, rk_ref, rv_ref, out_ref, level_ref, score_ref, *, kv_local):
    pipeline(roots(lambda f: stack_heads(q_ref, f * GROUP), rk_ref, rv_ref, range(kv_local), store(out_ref, level_ref)), score_ref)


def source_of(sources):
    me = lax.axis_index("seq").astype(jnp.int32)
    result = jnp.int32(sources[0])
    for device in range(1, len(sources)):
        result = jnp.where(me == device, sources[device], result)
    return result


def picks(pick_ref, sources, row_dev):
    source = source_of(sources)
    at = pl.ds(pl.multiple_of(source * row_dev, row_dev), row_dev)
    return [pick_ref[b, at, :] for b in range(pick_ref.shape[0])]


def merge(share_ref, pick, outputs, level, branch_ref, b_level):
    row_dev = level.shape[0]
    heads = len(outputs) * GROUP
    pick = jnp.concatenate(pick, axis=1)
    has = jnp.sum(pick.astype(jnp.float32), axis=1, keepdims=True) > 0.0
    found = dot(pick, b_level)
    b_level = jnp.where(has, found[:, :HEAD_DIM] + found[:, HEAD_DIM:2 * HEAD_DIM] + found[:, 2 * HEAD_DIM:], LOW)
    top = jnp.maximum(level, b_level)
    ours, theirs = jnp.exp2(level - top), jnp.exp2(b_level - top)
    both = ours + theirs
    ours, theirs = ours / both, theirs / both
    b_out = dot(pick, branch_ref[...])
    for f, output in enumerate(outputs):
        for g in range(GROUP):
            h = f * GROUP + g
            ahead = output[g * row_dev:(g + 1) * row_dev, :] * spread(ours, h, row_dev)
            share_ref[h * row_dev:(h + 1) * row_dev, :] = (ahead + b_out[:, h * HEAD_DIM:(h + 1) * HEAD_DIM] * spread(theirs, h, row_dev)).astype(jnp.bfloat16)
    write_level(share_ref, top + jnp.log2(both), heads)


def write_level(share_ref, level, heads):
    row_dev = level.shape[0]
    lane = lax.broadcasted_iota(jnp.int32, (row_dev, HEAD_DIM), 1)
    stat = jnp.where(lane < heads, level, 0.0)
    stat = stat + pltpu.roll(stat, heads, 1) + pltpu.roll(stat, 2 * heads, 1)
    hi, mid, low = [piece.astype(jnp.float32) for piece in pieces(stat)]
    packed = jnp.where(lane < heads, hi, jnp.where(lane < 2 * heads, mid, low))
    half = row_dev // 2
    share_ref[heads * row_dev:, :] = (packed[:half] + pltpu.roll(packed[half:], HEAD_DIM // 2, 1)).astype(jnp.bfloat16)


def branch(pick_ref, bias_ref, bk_ref, bv_ref, out_ref, level_ref, *rest, keys, direct, kv_local):
    q_refs, last_refs, rest = rest[:len(keys) - 1], rest[len(keys) - 1:-6], rest[-6:]
    share_ref, branch_ref, total_ref, last_ref, score_ref, rows_ref = rest
    row_dev, width = q_refs[0].shape
    branch_dev, _, most_rows = pick_ref.shape
    part = width // kv_local
    last = last_refs[0][...]
    if len(last_refs) > 1:
        last = jnp.where(source_of(direct) == 1, last, last_refs[1][...])
    last_ref[...] = last
    for sources, q_ref in zip(keys, [*q_refs, last_ref]):
        at = pl.ds(pl.multiple_of(source_of(sources) * row_dev, row_dev), row_dev)
        rows_ref[at, :] = q_ref[...]
    named = jnp.concatenate([pick_ref[b] for b in range(branch_dev)], axis=1)
    picked = dot(named, rows_ref[...], (((0,), (0,)), ((), ()))).astype(jnp.bfloat16)
    levels = [{} for _ in range(branch_dev)]

    def block(b, f):
        cut = slice(f * HEAD_DIM, (f + 1) * HEAD_DIM)

        def done(output, level):
            for h in range(GROUP):
                at = slice(f * part + h * HEAD_DIM, f * part + (h + 1) * HEAD_DIM)
                branch_ref[b * most_rows:(b + 1) * most_rows, at] = output[h * most_rows:(h + 1) * most_rows].astype(jnp.bfloat16)
            levels[b][f] = level

        return (lambda: stack_heads(picked[b * most_rows:(b + 1) * most_rows], f * GROUP), lambda at: bk_ref[b, at, cut], lambda at: bv_ref[b, at, cut], lambda at: bias_ref[b:b + 1, at], bk_ref.shape[1], done)

    pipeline([block(b, f) for b in range(branch_dev) for f in range(kv_local)], score_ref)
    total_ref[...] = jnp.concatenate(pieces(jnp.concatenate([compact(level) for level in levels], axis=0)), axis=1)
    merge(share_ref, picks(pick_ref, keys[1], row_dev), [out_ref[f] for f in range(kv_local)], level_ref[...], branch_ref, total_ref[...])


def share(pick_ref, b_level_ref, rk_ref, rv_ref, branch_ref, q_ref, share_ref, score_ref, *, key, kv_local):
    def finish(outputs, level):
        merge(share_ref, picks(pick_ref, key, level.shape[0]), list(outputs.values()), level, branch_ref, b_level_ref[...])

    pipeline(roots(lambda f: stack_heads(q_ref, f * GROUP), rk_ref, rv_ref, range(kv_local), finish), score_ref)


def given(pick_ref, b_level_ref, out_ref, level_ref, branch_ref, share_ref, *, key):
    merge(share_ref, picks(pick_ref, key, level_ref.shape[0]), [out_ref[f] for f in range(out_ref.shape[0])], level_ref[...], branch_ref, b_level_ref[...])


def join(*refs, heads):
    share_refs, out_ref = refs[:-1], refs[-1]
    row_dev = out_ref.shape[0]
    half = row_dev // 2
    levels = []
    for ref in share_refs:
        s = ref[heads * row_dev:, :].astype(jnp.float32)
        levels.append(s + pltpu.roll(s, HEAD_DIM - heads, 1) + pltpu.roll(s, HEAD_DIM - 2 * heads, 1))
    top = functools.reduce(jnp.maximum, levels)
    parts = [jnp.exp2(x - top) for x in levels]
    whole = functools.reduce(jnp.add, parts)
    parts = [x / whole for x in parts]
    for h in range(heads):
        result = None
        for ref, part in zip(share_refs, parts):
            factor = jnp.concatenate([spread(part, h, half), spread(part, HEAD_DIM // 2 + h, half)], axis=0)
            term = ref[h * row_dev:(h + 1) * row_dev, :].astype(jnp.float32) * factor
            result = term if result is None else result + term
        out_ref[:, h * HEAD_DIM:(h + 1) * HEAD_DIM] = result.astype(jnp.bfloat16)


VMEM = pl.BlockSpec(memory_space=pltpu.VMEM)
SMEM = pl.BlockSpec(memory_space=pltpu.SMEM)
HBM = pl.BlockSpec(memory_space=pltpu.HBM)


def call(kernel, out_shape, in_specs, scratch_shapes=(), **static):
    many = isinstance(out_shape, list)
    return pl.pallas_call(
        functools.partial(kernel, **static),
        out_shape=out_shape,
        in_specs=in_specs,
        out_specs=[VMEM] * len(out_shape) if many else VMEM,
        scratch_shapes=scratch_shapes,
        compiler_params=pltpu.CompilerParams(vmem_limit_bytes=VMEM_BYTES),
    )


def body(queries, root_keys, root_values, branch_keys, branch_values, branch_id, doc_len):
    shares = lax.axis_size("seq")
    row_dev, width = queries.shape
    rows = branch_id.shape[0]
    kv_local = root_keys.shape[1] // HEAD_DIM
    heads = kv_local * GROUP
    part = width // kv_local
    branch_dev, branch_len, _ = branch_keys.shape
    most_rows = 2 * row_dev // branch_dev
    slots = branch_dev * most_rows
    block = GROUP * row_dev
    f32 = functools.partial(jax.ShapeDtypeStruct, dtype=jnp.float32)
    bf16 = functools.partial(jax.ShapeDtypeStruct, dtype=jnp.bfloat16)
    scores = pltpu.VMEM((2, block, max(root_keys.shape[0], branch_len)), jnp.float32)
    some_rows = pltpu.VMEM((rows, part), jnp.bfloat16)
    result = [f32((kv_local, block, HEAD_DIM)), f32((row_dev, HEAD_DIM))]
    payload = bf16((heads * row_dev + row_dev // 2, HEAD_DIM))

    def move(x, targets):
        return lax.ppermute(x, "seq", [(i, target) for i, target in enumerate(targets) if target is not None])

    rounds, relay = plan(shares)
    back = [inverse(targets) for targets in rounds]
    early, last = range(len(rounds) - 1), len(rounds) - 1
    gathered = []
    for n in early:
        gathered.append(move(queries, rounds[n]))
    at_last = [move(queries, relay[0] if relay else rounds[last])]
    if relay:
        at_last.append(move(gathered[0], relay[1]))
    in_hbm = [pltpu.with_memory_space_constraint(x, pltpu.HBM) for x in (doc_len, branch_id.reshape(1, rows), root_keys, root_values, branch_keys, branch_values)]
    rk, rv, pick, bias = call(
        own,
        [bf16(x.shape) for x in (root_keys, root_values)] + [bf16((branch_dev, rows, most_rows)), f32((branch_dev, branch_len))],
        [HBM] * 4,
        [pltpu.VMEM((1, rows), jnp.int32), pltpu.SMEM(doc_len.shape, jnp.int32), pltpu.SemaphoreType.DMA((4,))],
    )(*in_hbm[:4])
    ready, branch_stored = [], []
    for n in early:
        if n < 2:
            *first, loaded = call(
                root_load, result + [bf16(branch_keys.shape)], [VMEM] * 3 + [HBM], [scores, pltpu.SemaphoreType.DMA(())], kv_local=kv_local
            )(gathered[n], rk, rv, in_hbm[4 + n])
            ready.append(first)
            branch_stored.append(loaded)
        else:
            ready.append(call(root, result, [VMEM] * 3, [scores], kv_local=kv_local)(gathered[n], rk, rv))
    bk, bv = branch_stored
    keys = [tuple(range(shares))] + back
    partial, out, total, rest = call(
        branch,
        [payload, bf16((slots, width)), bf16((slots, 3 * HEAD_DIM)), bf16((row_dev, width))],
        [VMEM] * (5 + shares + len(at_last)),
        [scores, pltpu.VMEM((rows, width), jnp.bfloat16)],
        keys=keys,
        direct=tuple(int(a == b) for a, b in zip(inverse(relay[0]), back[last])) if relay else None,
        kv_local=kv_local,
    )(pick, bias, bk, bv, *ready[0], queries, *gathered, *at_last)
    sent = [partial]
    for n in early[1:]:
        sent.append(call(given, payload, [VMEM] * 5, key=back[n])(pick, total, *ready[n], out))
    sent.append(call(share, payload, [VMEM] * 6, [scores], key=back[last], kv_local=kv_local)(pick, total, rk, rv, out, rest))
    received = [call(share, payload, [VMEM] * 6, [scores], key=keys[0], kv_local=kv_local)(pick, total, rk, rv, out, queries)]
    for n, partial in enumerate(sent):
        received.append(move(partial, back[n]))
    return call(join, bf16((row_dev, width)), [VMEM] * shares, heads=heads)(*received)


def inverse(targets):
    return tuple(targets.index(device) if device in targets else None for device in range(len(targets)))


def plan(shares):
    if shares == 4:
        return [(2, 0, 3, 1), (1, 3, 0, 2), (3, 2, 1, 0)], [(0, 2, 1, 3), (1, 0, 3, 2)]
    return [tuple(device ^ k for device in range(shares)) for k in range(1, shares)], None


def solution(mesh):
    rows = P(("parts", "seq"), "head")
    in_specs = (
        rows,
        rows,
        rows,
        P(("parts", "seq"), None, "head"),
        P(("parts", "seq"), None, "head"),
        P("parts", None),
        P("parts"),
    )

    return jax.shard_map(body, mesh=mesh, in_specs=in_specs, out_specs=rows, check_vma=False)
```

```python
import functools
import math

import jax
import jax.numpy as jnp
from jax import lax
from jax.experimental import pallas as pl
from jax.experimental.pallas import tpu as pltpu
from jax.sharding import PartitionSpec as P

QHEADS = 64
KVHEADS = 8
HEAD_DIM = 128
GROUP = QHEADS // KVHEADS
LOW = -1.0e30
SCALE = HEAD_DIM ** -0.5 * math.log2(math.e)
TILE = 512
VMEM_BYTES = 20 * 2 ** 20


def dot(a, b, dims=(((1,), (0,)), ((), ()))):
    return lax.dot_general(a, b, dims, preferred_element_type=jnp.float32)


def pieces(x):
    hi = x.astype(jnp.bfloat16)
    rest = x - hi.astype(jnp.float32)
    mid = rest.astype(jnp.bfloat16)
    low = (rest - mid.astype(jnp.float32)).astype(jnp.bfloat16)
    return hi, mid, low


def pipeline(blocks, score_ref):
    query, best = {}, {}

    def tiles(i):
        return [slice(at, at + TILE) for at in range(0, blocks[i][4], TILE)] if i < len(blocks) else []

    def score(i, at):
        if i not in query:
            query[i] = blocks[i][0]()
        s = dot(query[i], blocks[i][1](at), (((1,), (1,)), ((), ())))
        if blocks[i][3] is not None:
            s = s + blocks[i][3](at)
        score_ref[i % 2, :, at] = s
        for part in range(TILE // HEAD_DIM):
            t = s[:, part * HEAD_DIM:(part + 1) * HEAD_DIM]
            best[i] = jnp.maximum(best[i], t) if i in best else t

    for at in tiles(0):
        score(0, at)
    for i, (_, _, values, _, _, finish) in enumerate(blocks):
        peak = jnp.broadcast_to(jnp.max(best[i], axis=1, keepdims=True) * SCALE, best[i].shape)
        wide = jnp.concatenate([peak] * (TILE // HEAD_DIM), axis=1)
        ahead = tiles(i + 1)
        out = None
        for at in tiles(i):
            for later in ahead[:1]:
                score(i + 1, later)
            ahead = ahead[1:]
            w = jnp.exp2(score_ref[i % 2, :, at] * SCALE - wide).astype(jnp.bfloat16)
            part = dot(w, jnp.concatenate([values(at), jnp.ones((TILE, HEAD_DIM), jnp.bfloat16)], axis=1))
            out = part if out is None else out + part
        for later in ahead:
            score(i + 1, later)
        whole = out[:, HEAD_DIM:]
        finish(out[:, :HEAD_DIM] / whole, peak + jnp.log2(whole))


def stack_heads(chunk, first=0):
    return jnp.concatenate([chunk[:, (first + h) * HEAD_DIM:(first + h + 1) * HEAD_DIM] for h in range(GROUP)], axis=0)


def compact(levels):
    rows = next(iter(levels.values())).shape[0] // GROUP
    lane = lax.broadcasted_iota(jnp.int32, (rows, HEAD_DIM), 1)
    result = jnp.zeros((rows, HEAD_DIM), jnp.float32)
    for f, level in levels.items():
        for h in range(GROUP):
            result = jnp.where(lane == f * GROUP + h, level[h * rows:(h + 1) * rows, :], result)
    return result


def spread(stat, h, rows):
    return jnp.broadcast_to(stat[:, h:h + 1], (rows, HEAD_DIM))


def roots(query, rk_ref, rv_ref, heads, finish):
    outputs, levels = {}, {}

    def block(f):
        cut = slice(f * HEAD_DIM, (f + 1) * HEAD_DIM)

        def done(output, level):
            outputs[f], levels[f] = output, level
            if len(levels) == len(heads):
                finish(outputs, compact(levels))

        return (lambda: query(f), lambda at: rk_ref[at, cut], lambda at: rv_ref[at, cut], None, rk_ref.shape[0], done)

    return [block(f) for f in heads]


def store(out_ref, level_ref):
    def finish(outputs, level):
        for f, output in outputs.items():
            out_ref[f] = output
        level_ref[...] = level

    return finish


def own(doc_hbm, id_hbm, rk_hbm, rv_hbm, rk_ref, rv_ref, pick_ref, bias_ref, id_ref, doc_ref, arrived):
    loads = [pltpu.make_async_copy(source, target, arrived.at[n]) for n, (source, target) in enumerate(zip((doc_hbm, id_hbm, rk_hbm, rv_hbm), (doc_ref, id_ref, rk_ref, rv_ref)))]
    for load in loads:
        load.start()
    branch_dev, rows, most_rows = pick_ref.shape
    me = lax.axis_index("seq").astype(jnp.int32)
    loads[0].wait()
    slot = lax.broadcasted_iota(jnp.int32, (1, bias_ref.shape[1]), 1)
    for b in range(branch_dev):
        bias_ref[b:b + 1, :] = jnp.where(slot < doc_ref[me * branch_dev + b], 0.0, LOW)
    loads[1].wait()
    ids = id_ref[...]
    before = jnp.where(lax.broadcasted_iota(jnp.int32, (rows, rows), 0) < lax.broadcasted_iota(jnp.int32, (rows, rows), 1), 1.0, 0.0).astype(jnp.bfloat16)
    slot = lax.broadcasted_iota(jnp.int32, (most_rows, rows), 0).astype(jnp.float32)
    unit = jnp.where(lax.broadcasted_iota(jnp.int32, (most_rows, most_rows), 0) == lax.broadcasted_iota(jnp.int32, (most_rows, most_rows), 1), 1.0, 0.0).astype(jnp.bfloat16)
    for b in range(branch_dev):
        named = jnp.broadcast_to(jnp.where(ids == me * branch_dev + b, 1.0, 0.0), (most_rows, rows))
        rank = dot(named.astype(jnp.bfloat16), before)
        chosen = jnp.where((rank == slot) & (named > 0.0), 1.0, 0.0).astype(jnp.bfloat16)
        pick_ref[b] = dot(chosen, unit, (((0,), (0,)), ((), ()))).astype(jnp.bfloat16)
    for load in loads[2:]:
        load.wait()


def root_load(q_ref, rk_ref, rv_ref, stored_hbm, out_ref, level_ref, stored_ref, score_ref, arrived, *, kv_local):
    load = pltpu.make_async_copy(stored_hbm, stored_ref, arrived)
    load.start()
    root(q_ref, rk_ref, rv_ref, out_ref, level_ref, score_ref, kv_local=kv_local)
    load.wait()


def root(q_ref, rk_ref, rv_ref, out_ref, level_ref, score_ref, *, kv_local):
    pipeline(roots(lambda f: stack_heads(q_ref, f * GROUP), rk_ref, rv_ref, range(kv_local), store(out_ref, level_ref)), score_ref)


def source_of(sources):
    me = lax.axis_index("seq").astype(jnp.int32)
    result = jnp.int32(sources[0])
    for device in range(1, len(sources)):
        result = jnp.where(me == device, sources[device], result)
    return result


def picks(pick_ref, sources, row_dev):
    source = source_of(sources)
    at = pl.ds(pl.multiple_of(source * row_dev, row_dev), row_dev)
    return [pick_ref[b, at, :] for b in range(pick_ref.shape[0])]


def merge(share_ref, pick, outputs, level, branch_ref, b_level):
    row_dev = level.shape[0]
    heads = len(outputs) * GROUP
    pick = jnp.concatenate(pick, axis=1)
    has = jnp.sum(pick.astype(jnp.float32), axis=1, keepdims=True) > 0.0
    found = dot(pick, b_level)
    b_level = jnp.where(has, found[:, :HEAD_DIM] + found[:, HEAD_DIM:2 * HEAD_DIM] + found[:, 2 * HEAD_DIM:], LOW)
    top = jnp.maximum(level, b_level)
    ours, theirs = jnp.exp2(level - top), jnp.exp2(b_level - top)
    both = ours + theirs
    ours, theirs = ours / both, theirs / both
    b_out = dot(pick, branch_ref[...])
    for f, output in enumerate(outputs):
        for g in range(GROUP):
            h = f * GROUP + g
            ahead = output[g * row_dev:(g + 1) * row_dev, :] * spread(ours, h, row_dev)
            share_ref[h * row_dev:(h + 1) * row_dev, :] = (ahead + b_out[:, h * HEAD_DIM:(h + 1) * HEAD_DIM] * spread(theirs, h, row_dev)).astype(jnp.bfloat16)
    write_level(share_ref, top + jnp.log2(both), heads)


def write_level(share_ref, level, heads):
    row_dev = level.shape[0]
    lane = lax.broadcasted_iota(jnp.int32, (row_dev, HEAD_DIM), 1)
    stat = jnp.where(lane < heads, level, 0.0)
    stat = stat + pltpu.roll(stat, heads, 1) + pltpu.roll(stat, 2 * heads, 1)
    hi, mid, low = [piece.astype(jnp.float32) for piece in pieces(stat)]
    packed = jnp.where(lane < heads, hi, jnp.where(lane < 2 * heads, mid, low))
    half = row_dev // 2
    share_ref[heads * row_dev:, :] = (packed[:half] + pltpu.roll(packed[half:], HEAD_DIM // 2, 1)).astype(jnp.bfloat16)


def branch(pick_ref, bias_ref, bk_ref, bv_ref, out_ref, level_ref, *rest, keys, direct, kv_local):
    q_refs, last_refs, rest = rest[:len(keys) - 1], rest[len(keys) - 1:-6], rest[-6:]
    share_ref, branch_ref, total_ref, last_ref, score_ref, rows_ref = rest
    row_dev, width = q_refs[0].shape
    branch_dev, _, most_rows = pick_ref.shape
    part = width // kv_local
    last = last_refs[0][...]
    if len(last_refs) > 1:
        last = jnp.where(source_of(direct) == 1, last, last_refs[1][...])
    last_ref[...] = last
    for sources, q_ref in zip(keys, [*q_refs, last_ref]):
        at = pl.ds(pl.multiple_of(source_of(sources) * row_dev, row_dev), row_dev)
        rows_ref[at, :] = q_ref[...]
    named = jnp.concatenate([pick_ref[b] for b in range(branch_dev)], axis=1)
    picked = dot(named, rows_ref[...], (((0,), (0,)), ((), ()))).astype(jnp.bfloat16)
    levels = [{} for _ in range(branch_dev)]

    def block(b, f):
        cut = slice(f * HEAD_DIM, (f + 1) * HEAD_DIM)

        def done(output, level):
            for h in range(GROUP):
                at = slice(f * part + h * HEAD_DIM, f * part + (h + 1) * HEAD_DIM)
                branch_ref[b * most_rows:(b + 1) * most_rows, at] = output[h * most_rows:(h + 1) * most_rows].astype(jnp.bfloat16)
            levels[b][f] = level

        return (lambda: stack_heads(picked[b * most_rows:(b + 1) * most_rows], f * GROUP), lambda at: bk_ref[b, at, cut], lambda at: bv_ref[b, at, cut], lambda at: bias_ref[b:b + 1, at], bk_ref.shape[1], done)

    pipeline([block(b, f) for b in range(branch_dev) for f in range(kv_local)], score_ref)
    total_ref[...] = jnp.concatenate(pieces(jnp.concatenate([compact(level) for level in levels], axis=0)), axis=1)
    merge(share_ref, picks(pick_ref, keys[1], row_dev), [out_ref[f] for f in range(kv_local)], level_ref[...], branch_ref, total_ref[...])


def share(pick_ref, b_level_ref, rk_ref, rv_ref, branch_ref, q_ref, share_ref, score_ref, *, key, kv_local):
    def finish(outputs, level):
        merge(share_ref, picks(pick_ref, key, level.shape[0]), list(outputs.values()), level, branch_ref, b_level_ref[...])

    pipeline(roots(lambda f: stack_heads(q_ref, f * GROUP), rk_ref, rv_ref, range(kv_local), finish), score_ref)


def given(pick_ref, b_level_ref, out_ref, level_ref, branch_ref, share_ref, *, key):
    merge(share_ref, picks(pick_ref, key, level_ref.shape[0]), [out_ref[f] for f in range(out_ref.shape[0])], level_ref[...], branch_ref, b_level_ref[...])


def level_of(share_ref, heads, row_dev):
    s = share_ref[heads * row_dev:, :].astype(jnp.float32)
    return s + pltpu.roll(s, HEAD_DIM - heads, 1) + pltpu.roll(s, HEAD_DIM - 2 * heads, 1)


def combine(levels, refs, heads, row_dev, write):
    half = row_dev // 2
    top = functools.reduce(jnp.maximum, levels)
    parts = [jnp.exp2(x - top) for x in levels]
    whole = functools.reduce(jnp.add, parts)
    parts = [x / whole for x in parts]
    for h in range(heads):
        result = None
        for ref, part in zip(refs, parts):
            factor = jnp.concatenate([spread(part, h, half), spread(part, HEAD_DIM // 2 + h, half)], axis=0)
            term = ref[h * row_dev:(h + 1) * row_dev, :].astype(jnp.float32) * factor
            result = term if result is None else result + term
        write(h, result)
    return top + jnp.log2(whole)


def gather_up(*refs, heads, row_dev):
    share_refs, (sum_ref, level_ref) = refs[:-2], refs[-2:]

    def write(h, result):
        sum_ref[h * row_dev:(h + 1) * row_dev, :] = result

    level_ref[...] = combine([level_of(ref, heads, row_dev) for ref in share_refs], share_refs, heads, row_dev, write)


def join(sum_ref, level_ref, share_ref, out_ref, *, heads):
    row_dev = out_ref.shape[0]

    def write(h, result):
        out_ref[:, h * HEAD_DIM:(h + 1) * HEAD_DIM] = result.astype(jnp.bfloat16)

    combine([level_ref[...], level_of(share_ref, heads, row_dev)], [sum_ref, share_ref], heads, row_dev, write)


VMEM = pl.BlockSpec(memory_space=pltpu.VMEM)
SMEM = pl.BlockSpec(memory_space=pltpu.SMEM)
HBM = pl.BlockSpec(memory_space=pltpu.HBM)


def call(kernel, out_shape, in_specs, scratch_shapes=(), **static):
    many = isinstance(out_shape, list)
    return pl.pallas_call(
        functools.partial(kernel, **static),
        out_shape=out_shape,
        in_specs=in_specs,
        out_specs=[VMEM] * len(out_shape) if many else VMEM,
        scratch_shapes=scratch_shapes,
        compiler_params=pltpu.CompilerParams(vmem_limit_bytes=VMEM_BYTES),
    )


def body(queries, root_keys, root_values, branch_keys, branch_values, branch_id, doc_len):
    shares = lax.axis_size("seq")
    row_dev, width = queries.shape
    rows = branch_id.shape[0]
    kv_local = root_keys.shape[1] // HEAD_DIM
    heads = kv_local * GROUP
    part = width // kv_local
    branch_dev, branch_len, _ = branch_keys.shape
    most_rows = 2 * row_dev // branch_dev
    slots = branch_dev * most_rows
    block = GROUP * row_dev
    f32 = functools.partial(jax.ShapeDtypeStruct, dtype=jnp.float32)
    bf16 = functools.partial(jax.ShapeDtypeStruct, dtype=jnp.bfloat16)
    scores = pltpu.VMEM((2, block, max(root_keys.shape[0], branch_len)), jnp.float32)
    some_rows = pltpu.VMEM((rows, part), jnp.bfloat16)
    result = [f32((kv_local, block, HEAD_DIM)), f32((row_dev, HEAD_DIM))]
    payload = bf16((heads * row_dev + row_dev // 2, HEAD_DIM))

    def move(x, targets):
        return lax.ppermute(x, "seq", [(i, target) for i, target in enumerate(targets) if target is not None])

    rounds, relay = plan(shares)
    back = [inverse(targets) for targets in rounds]
    early, last = range(len(rounds) - 1), len(rounds) - 1
    gathered = []
    for n in early:
        gathered.append(move(queries, rounds[n]))
    at_last = [move(queries, relay[0] if relay else rounds[last])]
    if relay:
        at_last.append(move(gathered[0], relay[1]))
    in_hbm = [pltpu.with_memory_space_constraint(x, pltpu.HBM) for x in (doc_len, branch_id.reshape(1, rows), root_keys, root_values, branch_keys, branch_values)]
    rk, rv, pick, bias = call(
        own,
        [bf16(x.shape) for x in (root_keys, root_values)] + [bf16((branch_dev, rows, most_rows)), f32((branch_dev, branch_len))],
        [HBM] * 4,
        [pltpu.VMEM((1, rows), jnp.int32), pltpu.SMEM(doc_len.shape, jnp.int32), pltpu.SemaphoreType.DMA((4,))],
    )(*in_hbm[:4])
    ready, branch_stored = [], []
    for n in early:
        if n < 2:
            *first, loaded = call(
                root_load, result + [bf16(branch_keys.shape)], [VMEM] * 3 + [HBM], [scores, pltpu.SemaphoreType.DMA(())], kv_local=kv_local
            )(gathered[n], rk, rv, in_hbm[4 + n])
            ready.append(first)
            branch_stored.append(loaded)
        else:
            ready.append(call(root, result, [VMEM] * 3, [scores], kv_local=kv_local)(gathered[n], rk, rv))
    bk, bv = branch_stored
    keys = [tuple(range(shares))] + back
    partial, out, total, rest = call(
        branch,
        [payload, bf16((slots, width)), bf16((slots, 3 * HEAD_DIM)), bf16((row_dev, width))],
        [VMEM] * (5 + shares + len(at_last)),
        [scores, pltpu.VMEM((rows, width), jnp.bfloat16)],
        keys=keys,
        direct=tuple(int(a == b) for a, b in zip(inverse(relay[0]), back[last])) if relay else None,
        kv_local=kv_local,
    )(pick, bias, bk, bv, *ready[0], queries, *gathered, *at_last)
    sent = [partial]
    for n in early[1:]:
        sent.append(call(given, payload, [VMEM] * 5, key=back[n])(pick, total, *ready[n], out))
    sent.append(call(share, payload, [VMEM] * 6, [scores], key=back[last], kv_local=kv_local)(pick, total, rk, rv, out, rest))
    received = [call(share, payload, [VMEM] * 6, [scores], key=keys[0], kv_local=kv_local)(pick, total, rk, rv, out, queries)]
    for n, partial in enumerate(sent):
        received.append(move(partial, back[n]))
    added = call(gather_up, [f32((heads * row_dev, HEAD_DIM)), f32((row_dev // 2, HEAD_DIM))], [VMEM] * (shares - 1), heads=heads, row_dev=row_dev)(*received[:-1])
    return call(join, bf16((row_dev, width)), [VMEM] * 3, heads=heads)(*added, received[-1])


def inverse(targets):
    return tuple(targets.index(device) if device in targets else None for device in range(len(targets)))


def plan(shares):
    if shares == 4:
        return [(2, 0, 3, 1), (1, 3, 0, 2), (3, 2, 1, 0)], [(0, 2, 1, 3), (1, 0, 3, 2)]
    return [tuple(device ^ k for device in range(shares)) for k in range(1, shares)], None


def solution(mesh):
    rows = P(("parts", "seq"), "head")
    in_specs = (
        rows,
        rows,
        rows,
        P(("parts", "seq"), None, "head"),
        P(("parts", "seq"), None, "head"),
        P("parts", None),
        P("parts"),
    )

    return jax.shard_map(body, mesh=mesh, in_specs=in_specs, out_specs=rows, check_vma=False)
```

```python
import functools
import math

import jax
import jax.numpy as jnp
from jax import lax
from jax.experimental import pallas as pl
from jax.experimental.pallas import tpu as pltpu
from jax.sharding import PartitionSpec as P

QHEADS = 64
KVHEADS = 8
HEAD_DIM = 128
GROUP = QHEADS // KVHEADS
LOW = -1.0e30
SCALE = HEAD_DIM ** -0.5 * math.log2(math.e)
TILE = 512
VMEM_BYTES = 20 * 2 ** 20


def dot(a, b, dims=(((1,), (0,)), ((), ()))):
    return lax.dot_general(a, b, dims, preferred_element_type=jnp.float32)


def pieces(x):
    hi = x.astype(jnp.bfloat16)
    rest = x - hi.astype(jnp.float32)
    mid = rest.astype(jnp.bfloat16)
    low = (rest - mid.astype(jnp.float32)).astype(jnp.bfloat16)
    return hi, mid, low


def pipeline(blocks, score_ref):
    query, best = {}, {}

    def tiles(i):
        return [slice(at, at + TILE) for at in range(0, blocks[i][4], TILE)] if i < len(blocks) else []

    def score(i, at):
        if i not in query:
            query[i] = blocks[i][0]()
        s = dot(query[i], blocks[i][1](at), (((1,), (1,)), ((), ())))
        if blocks[i][3] is not None:
            s = s + blocks[i][3](at)
        score_ref[i % 2, :, at] = s
        for part in range(TILE // HEAD_DIM):
            t = s[:, part * HEAD_DIM:(part + 1) * HEAD_DIM]
            best[i] = jnp.maximum(best[i], t) if i in best else t

    for at in tiles(0):
        score(0, at)
    for i, (_, _, values, _, _, finish) in enumerate(blocks):
        peak = jnp.broadcast_to(jnp.max(best[i], axis=1, keepdims=True) * SCALE, best[i].shape)
        wide = jnp.concatenate([peak] * (TILE // HEAD_DIM), axis=1)
        ahead = tiles(i + 1)
        out = None
        for at in tiles(i):
            for later in ahead[:1]:
                score(i + 1, later)
            ahead = ahead[1:]
            w = jnp.exp2(score_ref[i % 2, :, at] * SCALE - wide).astype(jnp.bfloat16)
            part = dot(w, jnp.concatenate([values(at), jnp.ones((TILE, HEAD_DIM), jnp.bfloat16)], axis=1))
            out = part if out is None else out + part
        for later in ahead:
            score(i + 1, later)
        whole = out[:, HEAD_DIM:]
        finish(out[:, :HEAD_DIM] / whole, peak + jnp.log2(whole))


def stack_heads(chunk, first=0):
    return jnp.concatenate([chunk[:, (first + h) * HEAD_DIM:(first + h + 1) * HEAD_DIM] for h in range(GROUP)], axis=0)


def compact(levels):
    rows = next(iter(levels.values())).shape[0] // GROUP
    lane = lax.broadcasted_iota(jnp.int32, (rows, HEAD_DIM), 1)
    result = jnp.zeros((rows, HEAD_DIM), jnp.float32)
    for f, level in levels.items():
        for h in range(GROUP):
            result = jnp.where(lane == f * GROUP + h, level[h * rows:(h + 1) * rows, :], result)
    return result


def spread(stat, h, rows):
    return jnp.broadcast_to(stat[:, h:h + 1], (rows, HEAD_DIM))


def roots(query, rk_ref, rv_ref, heads, finish):
    outputs, levels = {}, {}

    def block(f):
        cut = slice(f * HEAD_DIM, (f + 1) * HEAD_DIM)

        def done(output, level):
            outputs[f], levels[f] = output, level
            if len(levels) == len(heads):
                finish(outputs, compact(levels))

        return (lambda: query(f), lambda at: rk_ref[at, cut], lambda at: rv_ref[at, cut], None, rk_ref.shape[0], done)

    return [block(f) for f in heads]


def store(out_ref, level_ref):
    def finish(outputs, level):
        for f, output in outputs.items():
            out_ref[f] = output
        level_ref[...] = level

    return finish


def own(doc_hbm, id_hbm, rk_hbm, rv_hbm, rk_ref, rv_ref, pick_ref, bias_ref, id_ref, doc_ref, arrived):
    loads = [pltpu.make_async_copy(source, target, arrived.at[n]) for n, (source, target) in enumerate(zip((doc_hbm, id_hbm, rk_hbm, rv_hbm), (doc_ref, id_ref, rk_ref, rv_ref)))]
    for load in loads:
        load.start()
    branch_dev, rows, most_rows = pick_ref.shape
    me = lax.axis_index("seq").astype(jnp.int32)
    loads[0].wait()
    slot = lax.broadcasted_iota(jnp.int32, (1, bias_ref.shape[1]), 1)
    for b in range(branch_dev):
        bias_ref[b:b + 1, :] = jnp.where(slot < doc_ref[me * branch_dev + b], 0.0, LOW)
    loads[1].wait()
    ids = id_ref[...]
    before = jnp.where(lax.broadcasted_iota(jnp.int32, (rows, rows), 0) < lax.broadcasted_iota(jnp.int32, (rows, rows), 1), 1.0, 0.0).astype(jnp.bfloat16)
    slot = lax.broadcasted_iota(jnp.int32, (most_rows, rows), 0).astype(jnp.float32)
    unit = jnp.where(lax.broadcasted_iota(jnp.int32, (most_rows, most_rows), 0) == lax.broadcasted_iota(jnp.int32, (most_rows, most_rows), 1), 1.0, 0.0).astype(jnp.bfloat16)
    for b in range(branch_dev):
        named = jnp.broadcast_to(jnp.where(ids == me * branch_dev + b, 1.0, 0.0), (most_rows, rows))
        rank = dot(named.astype(jnp.bfloat16), before)
        chosen = jnp.where((rank == slot) & (named > 0.0), 1.0, 0.0).astype(jnp.bfloat16)
        pick_ref[b] = dot(chosen, unit, (((0,), (0,)), ((), ()))).astype(jnp.bfloat16)
    for load in loads[2:]:
        load.wait()


def root_load(q_ref, rk_ref, rv_ref, stored_hbm, out_ref, level_ref, stored_ref, score_ref, arrived, *, kv_local):
    load = pltpu.make_async_copy(stored_hbm, stored_ref, arrived)
    load.start()
    root(q_ref, rk_ref, rv_ref, out_ref, level_ref, score_ref, kv_local=kv_local)
    load.wait()


def root(q_ref, rk_ref, rv_ref, out_ref, level_ref, score_ref, *, kv_local):
    pipeline(roots(lambda f: stack_heads(q_ref, f * GROUP), rk_ref, rv_ref, range(kv_local), store(out_ref, level_ref)), score_ref)


def source_of(sources):
    me = lax.axis_index("seq").astype(jnp.int32)
    result = jnp.int32(sources[0])
    for device in range(1, len(sources)):
        result = jnp.where(me == device, sources[device], result)
    return result


def picks(pick_ref, sources, row_dev):
    source = source_of(sources)
    at = pl.ds(pl.multiple_of(source * row_dev, row_dev), row_dev)
    return [pick_ref[b, at, :] for b in range(pick_ref.shape[0])]


def merge_head(share_ref, pick, has, f, output, level, branch_ref, b_level):
    row_dev = level.shape[0]
    found = dot(pick, b_level)
    b_level = jnp.where(has, found[:, :HEAD_DIM] + found[:, HEAD_DIM:2 * HEAD_DIM] + found[:, 2 * HEAD_DIM:], LOW)
    top = jnp.maximum(level, b_level)
    ours, theirs = jnp.exp2(level - top), jnp.exp2(b_level - top)
    both = ours + theirs
    ours, theirs = ours / both, theirs / both
    b_out = dot(pick, branch_ref[:, f * GROUP * HEAD_DIM:(f + 1) * GROUP * HEAD_DIM])
    for g in range(GROUP):
        h = f * GROUP + g
        ahead = output[g * row_dev:(g + 1) * row_dev, :] * spread(ours, h, row_dev)
        share_ref[h * row_dev:(h + 1) * row_dev, :] = (ahead + b_out[:, g * HEAD_DIM:(g + 1) * HEAD_DIM] * spread(theirs, h, row_dev)).astype(jnp.bfloat16)
    return top + jnp.log2(both)


def named_rows(pick):
    pick = jnp.concatenate(pick, axis=1)
    return pick, jnp.sum(pick.astype(jnp.float32), axis=1, keepdims=True) > 0.0


def write_levels(share_ref, levels):
    lane = lax.broadcasted_iota(jnp.int32, levels[0].shape, 1)
    level = levels[0]
    for f in range(1, len(levels)):
        level = jnp.where(lane >= f * GROUP, levels[f], level)
    write_level(share_ref, level, len(levels) * GROUP)


def merge(share_ref, pick, outputs, level, branch_ref, b_level):
    pick, has = named_rows(pick)
    write_levels(share_ref, [merge_head(share_ref, pick, has, f, output, level, branch_ref, b_level) for f, output in enumerate(outputs)])


def write_level(share_ref, level, heads):
    row_dev = level.shape[0]
    lane = lax.broadcasted_iota(jnp.int32, (row_dev, HEAD_DIM), 1)
    stat = jnp.where(lane < heads, level, 0.0)
    stat = stat + pltpu.roll(stat, heads, 1) + pltpu.roll(stat, 2 * heads, 1)
    hi, mid, low = [piece.astype(jnp.float32) for piece in pieces(stat)]
    packed = jnp.where(lane < heads, hi, jnp.where(lane < 2 * heads, mid, low))
    half = row_dev // 2
    share_ref[heads * row_dev:, :] = (packed[:half] + pltpu.roll(packed[half:], HEAD_DIM // 2, 1)).astype(jnp.bfloat16)


def branch(pick_ref, bias_ref, bk_ref, bv_ref, out_ref, level_ref, *rest, keys, direct, kv_local):
    q_refs, last_refs, rest = rest[:len(keys) - 1], rest[len(keys) - 1:-6], rest[-6:]
    share_ref, branch_ref, total_ref, last_ref, score_ref, rows_ref = rest
    row_dev, width = q_refs[0].shape
    branch_dev, _, most_rows = pick_ref.shape
    part = width // kv_local
    last = last_refs[0][...]
    if len(last_refs) > 1:
        last = jnp.where(source_of(direct) == 1, last, last_refs[1][...])
    last_ref[...] = last
    for sources, q_ref in zip(keys, [*q_refs, last_ref]):
        at = pl.ds(pl.multiple_of(source_of(sources) * row_dev, row_dev), row_dev)
        rows_ref[at, :] = q_ref[...]
    named = jnp.concatenate([pick_ref[b] for b in range(branch_dev)], axis=1)
    picked = dot(named, rows_ref[...], (((0,), (0,)), ((), ()))).astype(jnp.bfloat16)
    levels = [{} for _ in range(branch_dev)]

    def block(b, f):
        cut = slice(f * HEAD_DIM, (f + 1) * HEAD_DIM)

        def done(output, level):
            for h in range(GROUP):
                at = slice(f * part + h * HEAD_DIM, f * part + (h + 1) * HEAD_DIM)
                branch_ref[b * most_rows:(b + 1) * most_rows, at] = output[h * most_rows:(h + 1) * most_rows].astype(jnp.bfloat16)
            levels[b][f] = level

        return (lambda: stack_heads(picked[b * most_rows:(b + 1) * most_rows], f * GROUP), lambda at: bk_ref[b, at, cut], lambda at: bv_ref[b, at, cut], lambda at: bias_ref[b:b + 1, at], bk_ref.shape[1], done)

    pipeline([block(b, f) for b in range(branch_dev) for f in range(kv_local)], score_ref)
    total_ref[...] = jnp.concatenate(pieces(jnp.concatenate([compact(level) for level in levels], axis=0)), axis=1)
    merge(share_ref, picks(pick_ref, keys[1], row_dev), [out_ref[f] for f in range(kv_local)], level_ref[...], branch_ref, total_ref[...])


def share(pick_ref, b_level_ref, rk_ref, rv_ref, branch_ref, q_ref, share_ref, score_ref, *, key, kv_local):
    pick, has = named_rows(picks(pick_ref, key, q_ref.shape[0]))
    joined = []

    def finish(outputs, level):
        for f, output in outputs.items():
            joined.append(merge_head(share_ref, pick, has, f, output, level, branch_ref, b_level_ref[...]))

    blocks = [roots(lambda f: stack_heads(q_ref, f * GROUP), rk_ref, rv_ref, [f], finish)[0] for f in range(kv_local)]
    pipeline(blocks, score_ref)
    write_levels(share_ref, joined)


def given(pick_ref, b_level_ref, out_ref, level_ref, branch_ref, share_ref, *, key):
    merge(share_ref, picks(pick_ref, key, level_ref.shape[0]), [out_ref[f] for f in range(out_ref.shape[0])], level_ref[...], branch_ref, b_level_ref[...])


def level_of(share_ref, heads, row_dev):
    s = share_ref[heads * row_dev:, :].astype(jnp.float32)
    return s + pltpu.roll(s, HEAD_DIM - heads, 1) + pltpu.roll(s, HEAD_DIM - 2 * heads, 1)


def combine(levels, refs, heads, row_dev, write):
    half = row_dev // 2
    top = functools.reduce(jnp.maximum, levels)
    parts = [jnp.exp2(x - top) for x in levels]
    whole = functools.reduce(jnp.add, parts)
    parts = [x / whole for x in parts]
    for h in range(heads):
        result = None
        for ref, part in zip(refs, parts):
            factor = jnp.concatenate([spread(part, h, half), spread(part, HEAD_DIM // 2 + h, half)], axis=0)
            term = ref[h * row_dev:(h + 1) * row_dev, :].astype(jnp.float32) * factor
            result = term if result is None else result + term
        write(h, result)
    return top + jnp.log2(whole)


def gather_up(*refs, heads, row_dev):
    share_refs, (sum_ref, level_ref) = refs[:-2], refs[-2:]

    def write(h, result):
        sum_ref[h * row_dev:(h + 1) * row_dev, :] = result

    level_ref[...] = combine([level_of(ref, heads, row_dev) for ref in share_refs], share_refs, heads, row_dev, write)


def join(sum_ref, level_ref, share_ref, out_ref, *, heads):
    row_dev = out_ref.shape[0]

    def write(h, result):
        out_ref[:, h * HEAD_DIM:(h + 1) * HEAD_DIM] = result.astype(jnp.bfloat16)

    combine([level_ref[...], level_of(share_ref, heads, row_dev)], [sum_ref, share_ref], heads, row_dev, write)


VMEM = pl.BlockSpec(memory_space=pltpu.VMEM)
SMEM = pl.BlockSpec(memory_space=pltpu.SMEM)
HBM = pl.BlockSpec(memory_space=pltpu.HBM)


def call(kernel, out_shape, in_specs, scratch_shapes=(), **static):
    many = isinstance(out_shape, list)
    return pl.pallas_call(
        functools.partial(kernel, **static),
        out_shape=out_shape,
        in_specs=in_specs,
        out_specs=[VMEM] * len(out_shape) if many else VMEM,
        scratch_shapes=scratch_shapes,
        compiler_params=pltpu.CompilerParams(vmem_limit_bytes=VMEM_BYTES),
    )


def body(queries, root_keys, root_values, branch_keys, branch_values, branch_id, doc_len):
    shares = lax.axis_size("seq")
    row_dev, width = queries.shape
    rows = branch_id.shape[0]
    kv_local = root_keys.shape[1] // HEAD_DIM
    heads = kv_local * GROUP
    part = width // kv_local
    branch_dev, branch_len, _ = branch_keys.shape
    most_rows = 2 * row_dev // branch_dev
    slots = branch_dev * most_rows
    block = GROUP * row_dev
    f32 = functools.partial(jax.ShapeDtypeStruct, dtype=jnp.float32)
    bf16 = functools.partial(jax.ShapeDtypeStruct, dtype=jnp.bfloat16)
    scores = pltpu.VMEM((2, block, max(root_keys.shape[0], branch_len)), jnp.float32)
    some_rows = pltpu.VMEM((rows, part), jnp.bfloat16)
    result = [f32((kv_local, block, HEAD_DIM)), f32((row_dev, HEAD_DIM))]
    payload = bf16((heads * row_dev + row_dev // 2, HEAD_DIM))

    def move(x, targets):
        return lax.ppermute(x, "seq", [(i, target) for i, target in enumerate(targets) if target is not None])

    rounds, relay = plan(shares)
    back = [inverse(targets) for targets in rounds]
    early, last = range(len(rounds) - 1), len(rounds) - 1
    gathered = []
    for n in early:
        gathered.append(move(queries, rounds[n]))
    at_last = [move(queries, relay[0] if relay else rounds[last])]
    if relay:
        at_last.append(move(gathered[0], relay[1]))
    in_hbm = [pltpu.with_memory_space_constraint(x, pltpu.HBM) for x in (doc_len, branch_id.reshape(1, rows), root_keys, root_values, branch_keys, branch_values)]
    rk, rv, pick, bias = call(
        own,
        [bf16(x.shape) for x in (root_keys, root_values)] + [bf16((branch_dev, rows, most_rows)), f32((branch_dev, branch_len))],
        [HBM] * 4,
        [pltpu.VMEM((1, rows), jnp.int32), pltpu.SMEM(doc_len.shape, jnp.int32), pltpu.SemaphoreType.DMA((4,))],
    )(*in_hbm[:4])
    ready, branch_stored = [], []
    for n in early:
        if n < 2:
            *first, loaded = call(
                root_load, result + [bf16(branch_keys.shape)], [VMEM] * 3 + [HBM], [scores, pltpu.SemaphoreType.DMA(())], kv_local=kv_local
            )(gathered[n], rk, rv, in_hbm[4 + n])
            ready.append(first)
            branch_stored.append(loaded)
        else:
            ready.append(call(root, result, [VMEM] * 3, [scores], kv_local=kv_local)(gathered[n], rk, rv))
    bk, bv = branch_stored
    keys = [tuple(range(shares))] + back
    partial, out, total, rest = call(
        branch,
        [payload, bf16((slots, width)), bf16((slots, 3 * HEAD_DIM)), bf16((row_dev, width))],
        [VMEM] * (5 + shares + len(at_last)),
        [scores, pltpu.VMEM((rows, width), jnp.bfloat16)],
        keys=keys,
        direct=tuple(int(a == b) for a, b in zip(inverse(relay[0]), back[last])) if relay else None,
        kv_local=kv_local,
    )(pick, bias, bk, bv, *ready[0], queries, *gathered, *at_last)
    sent = [partial]
    for n in early[1:]:
        sent.append(call(given, payload, [VMEM] * 5, key=back[n])(pick, total, *ready[n], out))
    sent.append(call(share, payload, [VMEM] * 6, [scores], key=back[last], kv_local=kv_local)(pick, total, rk, rv, out, rest))
    received = [call(share, payload, [VMEM] * 6, [scores], key=keys[0], kv_local=kv_local)(pick, total, rk, rv, out, queries)]
    for n, partial in enumerate(sent):
        received.append(move(partial, back[n]))
    added = call(gather_up, [f32((heads * row_dev, HEAD_DIM)), f32((row_dev // 2, HEAD_DIM))], [VMEM] * (shares - 1), heads=heads, row_dev=row_dev)(*received[:-1])
    return call(join, bf16((row_dev, width)), [VMEM] * 3, heads=heads)(*added, received[-1])


def inverse(targets):
    return tuple(targets.index(device) if device in targets else None for device in range(len(targets)))


def plan(shares):
    if shares == 4:
        return [(2, 0, 3, 1), (1, 3, 0, 2), (3, 2, 1, 0)], [(0, 2, 1, 3), (1, 0, 3, 2)]
    return [tuple(device ^ k for device in range(shares)) for k in range(1, shares)], None


def solution(mesh):
    rows = P(("parts", "seq"), "head")
    in_specs = (
        rows,
        rows,
        rows,
        P(("parts", "seq"), None, "head"),
        P(("parts", "seq"), None, "head"),
        P("parts", None),
        P("parts"),
    )

    return jax.shard_map(body, mesh=mesh, in_specs=in_specs, out_specs=rows, check_vma=False)
```
